32 devices in a mesh: ctx: 4 (over z), exp: 8 (over y, x, core).
Axes of the slice: x: 2, y: 2, z: 4, core: 2. Of those that a mesh axis runs over, the one named last changes fastest.
Arguments:
- seq_inputs: bfloat16 [2048, 2048], P('ctx', 'exp'), may hold values from -6 to 6
- step_size: float32 [32, 2048], P('exp', 'ctx'), may hold values from 0.0007 to 0.14
- write_map: bfloat16 [16, 2048], P(None, 'ctx'), may hold values from -2 to 2
- read_map: bfloat16 [16, 2048], P(None, 'ctx'), may hold values from -2 to 2
- decay_log: float32 [32], P('exp'), may hold values from -9.3 to 1.4
- skip_gain: float32 [32], P('exp'), may hold values from 0.5 to 1.5
- moe_tokens: bfloat16 [1024, 4096], P('exp'), may hold values from -6 to 6
- expert_ids: int32 [1024, 2], P('exp'), may hold values from 0 to 3, all different within a row; in each aligned block of 128 rows (0 to 127, 128 to 255, ...) at most 128 rows name the same one
- route_weights: float32 [1024, 2], P('exp'), may hold values from 0.1 to 1
- gate_proj: bfloat16 [8, 4096, 3584], P('exp', None, 'ctx'), may hold values from -0.09375 to 0.09375
- up_proj: bfloat16 [8, 4096, 3584], P('exp', None, 'ctx'), may hold values from -0.09375 to 0.09375
- down_proj: bfloat16 [8, 3584, 4096], P('exp', None, 'ctx'), may hold values from -0.0625 to 0.0625
Outputs:
- mixer_output: bfloat16 [2048, 2048], P('ctx', 'exp')
- expert_output: bfloat16 [1024, 4096], P('exp', 'ctx')
The draws below stay inside these ranges and needn't reach their ends.
Inputs may be any that keep to these rules, and one draw needn't show every extreme that they name: `expert_ids`: each row names two different experts. In the 128 rows of one index of exp (aligned blocks), no expert is named more than 128 times, and in some blocks an expert is named exactly 128 times.
All inputs are finite; a program needn't handle non-finite values.
Results may differ from the reference program's by a relative error of at most 0.002.
The reference program's roundings to bfloat16 on the way count: a program that leaves them out, or rounds other values in their place, can miss the bound.
Values may be sent and summed in bfloat16 or wider, within the bound.
A program may use at most 64 MiB of HBM per device.

```python
import math
import jax
import jax.numpy as jnp
import numpy as np
from jax import lax

D = 4096
FF = 7168
EXPERTS = 4
MOE_DEV = 128
MOE_TOKENS = 1024
CAP = 128
HEADS = 32
HEAD_SIZE = 64
STATE = 16
BLOCK = 256
SEQ = 2048
N_EXP = 8


def draw_step_size(key, part):
    first, second = jax.random.split(key)
    base = jax.random.uniform(first, (HEADS, SEQ), jnp.float32, math.log(0.002), math.log(0.05))
    region = jax.random.uniform(second, (HEADS, SEQ // BLOCK), jnp.float32, -1.0, 1.0)
    return jnp.exp(base + jnp.repeat(region, BLOCK, axis=1)).astype(jnp.float32)


def draw_decay_log(key, part):
    first, second, third = jax.random.split(key, 3)
    share = 0.5
    keeping = jax.random.bernoulli(first, share, (HEADS,))
    slower = jax.random.uniform(second, (HEADS,), jnp.float32, math.log(0.0001), math.log(0.0004))
    faster = jax.random.uniform(third, (HEADS,), jnp.float32, 0.0, math.log(4.0))
    return jnp.where(keeping, slower, faster).astype(jnp.float32)


def block_levels(key, shape, cuts, least, high):
    gain, own = 1.0, jax.random.fold_in(key, 6)
    for position, parts in cuts:
        draws = jnp.exp(jax.random.uniform(jax.random.fold_in(own, position), (parts,), jnp.float32, least / len(cuts), high / len(cuts)))
        gain = gain * jnp.repeat(draws, shape[position] // parts).reshape([-1 if axis == position else 1 for axis in range(len(shape))])
    return gain


def deal_out(rng, own, number, rows, count, top, bound, lean):
    ranking = jax.random.permutation(rng, count)
    crowded, ordinary = shares(count, rows * top, bound, lean, True), shares(count, rows * top, bound, lean, False)
    places = jnp.arange(count)

    def named(tallies, turn):
        used = int((tallies > 0).sum())
        fixed = max(1, used // 4)
        shifted = fixed + (places - fixed + turn * (used - fixed)) % max(1, count - fixed)
        return jnp.zeros((count,), jnp.int32).at[ranking[jnp.where(places < fixed, places, shifted)]].set(jnp.asarray(tallies, jnp.int32))

    tallies = jnp.where(number % 4 == 0, named(crowded, number // 4), named(ordinary, number - number // 4 - 1))
    mixed = jax.random.permutation(jax.random.fold_in(own, 3), count)
    source_of, sink = mixed[0:count // 2 * 2:2], mixed[1:count // 2 * 2:2]
    room = jnp.minimum(tallies[source_of] - 1, bound - tallies[sink]) // 2
    room = jnp.where((source_of == ranking[0]) | (sink == ranking[0]) | (tallies[sink] == 0), 0, jnp.maximum(room, 0))
    shifted = jax.random.randint(jax.random.fold_in(own, 4), (count // 2,), 0, 1 << 20) % (room + 1)
    tallies = tallies.at[source_of].add(-shifted).at[sink].add(shifted)
    labels = jnp.searchsorted(jnp.cumsum(tallies), jnp.arange(rows * top), side="right").astype(jnp.int32)
    table = labels.reshape(top, rows).T
    table = table[jax.random.permutation(jax.random.fold_in(own, 1), rows)]
    turn = jax.random.randint(jax.random.fold_in(own, 2), (rows, 1), 0, top)
    return jnp.take_along_axis(table, (jnp.arange(top)[None, :] + turn) % top, axis=1)


def shares(number_of, total, most, slope, full):
    weights = [(1 << 20) // math.isqrt(grade ** slope) + 1 for grade in range(1, number_of + 1)]
    largest = most if full else min(most, max(-(-total // number_of), total * weights[0] // sum(weights)))
    least = 1 if total - largest >= number_of - 1 else 0
    counts, surplus = [largest] + [least] * (number_of - 1), total - largest - least * (number_of - 1)
    while surplus > 0:
        movable = [i for i in range(1, number_of) if counts[i] < largest] or [i for i in range(1, number_of) if counts[i] < most]
        mass, remaining = sum([weights[i] for i in movable]), surplus
        for i in movable:
            extra = min(most - counts[i], max(1, remaining * weights[i] // mass), surplus)
            counts[i] = counts[i] + extra
            surplus = surplus - extra
    return np.array(counts)


def bell_draw(key, extent, width, reach, cuts=(), kind=jnp.bfloat16):
    array = jax.random.normal(key, extent, jnp.float32) * width
    if len(cuts) > 0:
        array = block_levels(key, extent, cuts, -0.22, 0.18) * array
    return jnp.clip(array, min=-reach, max=reach).astype(kind)


def setup_inputs(seed: int = 0) -> dict:
    key_list = jax.random.split(jax.random.key(seed), 13)
    seq_inputs = bell_draw(key_list[0], (SEQ, HEADS * HEAD_SIZE), 1.0, 6.0, ((0, 4), (1, 8)))
    step_size = draw_step_size(jax.random.fold_in(key_list[12], 71), 0)
    write_map = bell_draw(key_list[2], (STATE, SEQ), 0.3, 2.0, ((1, 4),))
    read_map = bell_draw(key_list[3], (STATE, SEQ), 0.3, 2.0, ((1, 4),))
    decay_log = draw_decay_log(jax.random.fold_in(key_list[12], 71), 0)
    skip_gain = jnp.clip(0.5 + 1.0 * jax.random.uniform(key_list[5], (HEADS,), jnp.float32) ** block_levels(key_list[5], (HEADS,), ((0, 8),), -0.2, 0.2), 0.5, 1.5)
    moe_tokens = bell_draw(key_list[6], (MOE_TOKENS, D), 1.0, 6.0, ((0, 8),))
    expert_ids_keys = jax.random.split(jax.random.fold_in(key_list[7], 1), MOE_TOKENS // MOE_DEV)
    expert_ids_turns = jax.random.permutation(jax.random.fold_in(key_list[7], 3), MOE_TOKENS // MOE_DEV)
    expert_ids = jax.vmap(lambda own, number: deal_out(jax.random.fold_in(key_list[7], 2), own, number, MOE_DEV, EXPERTS, 2, CAP, 2))(expert_ids_keys, expert_ids_turns).reshape((MOE_TOKENS, 2))
    route_weights = jnp.clip(0.1 + 0.9 * jax.random.uniform(key_list[8], (MOE_TOKENS, 2), jnp.float32) ** block_levels(key_list[8], (MOE_TOKENS, 2), ((0, 8),), -0.2, 0.2), 0.1, 1.0)
    gate_proj = bell_draw(key_list[9], (2 * EXPERTS, D, FF // 2), D ** -0.5, 0.09375, ((0, 8), (2, 4)))
    up_proj = bell_draw(key_list[10], (2 * EXPERTS, D, FF // 2), D ** -0.5, 0.09375, ((0, 8), (2, 4)))
    down_proj = bell_draw(key_list[11], (2 * EXPERTS, FF // 2, D), FF ** -0.5, 0.0625, ((0, 8), (2, 4)))
    return dict(seq_inputs=seq_inputs, step_size=step_size, write_map=write_map, read_map=read_map, decay_log=decay_log, skip_gain=skip_gain, moe_tokens=moe_tokens, expert_ids=expert_ids, route_weights=route_weights, gate_proj=gate_proj, up_proj=up_proj, down_proj=down_proj)


HIGHEST = lax.Precision.HIGHEST


def mixer_reference(seq_inputs, step_size, write_map, read_map, decay_log, skip_gain):
    length = seq_inputs.shape[0]
    head_count = step_size.shape[0]
    state_count = write_map.shape[0]
    head_width = seq_inputs.shape[1] // head_count
    block_count = length // BLOCK
    decay_rate = -jnp.exp(decay_log)
    log_decay = (step_size * decay_rate[:, None]).reshape(head_count, block_count, BLOCK).transpose(1, 0, 2)
    step_blocks = step_size.reshape(head_count, block_count, BLOCK).transpose(1, 0, 2)
    write_blocks = write_map.reshape(state_count, block_count, BLOCK).transpose(1, 0, 2)
    read_blocks = read_map.reshape(state_count, block_count, BLOCK).transpose(1, 0, 2)
    value_blocks = seq_inputs.reshape(block_count, BLOCK, head_count, head_width)
    row_index = lax.broadcasted_iota(jnp.int32, (BLOCK, BLOCK), 0)
    column_index = lax.broadcasted_iota(jnp.int32, (BLOCK, BLOCK), 1)
    lower = column_index <= row_index

    def one_block(running, pieces):
        log_part, step_part, write_part, read_part, value_part = pieces
        cumulative = jnp.cumsum(log_part, axis=1)
        block_end = cumulative[:, BLOCK - 1]
        scores = jnp.dot(read_part.T, write_part, preferred_element_type=jnp.float32)
        difference = cumulative[:, :, None] - cumulative[:, None, :]
        decay = jnp.where(lower[None], jnp.exp(jnp.minimum(difference, 0.0)), 0.0)
        mixing = (scores[None] * decay * step_part[:, None, :]).astype(jnp.bfloat16)
        values = value_part.astype(jnp.float32)
        local_mix = jnp.einsum("hts,shp->thp", mixing.astype(jnp.float32), values)
        carried = jnp.einsum("nt,hnp->thp", read_part.astype(jnp.float32), running, precision=HIGHEST)
        carried = carried * jnp.exp(cumulative).T[:, :, None]
        output = local_mix + carried + skip_gain[None, :, None] * values
        weights = jnp.exp(block_end[:, None] - cumulative) * step_part
        key_decayed = (write_part[None] * weights[:, None, :]).astype(jnp.bfloat16)
        increment = jnp.einsum("hns,shp->hnp", key_decayed.astype(jnp.float32), values)
        running = jnp.exp(block_end)[:, None, None] * running + increment
        return running, output.astype(jnp.bfloat16)

    zero_state = jnp.zeros((head_count, state_count, head_width), jnp.float32)
    final_state, outputs = lax.scan(one_block, zero_state, (log_decay, step_blocks, write_blocks, read_blocks, value_blocks))
    return outputs.reshape(length, head_count * head_width)


def expert_reference(moe_tokens, expert_ids, route_weights, gate_proj, up_proj, down_proj):
    total_tokens = moe_tokens.shape[0]
    model_width = moe_tokens.shape[1]
    group_size = total_tokens // N_EXP
    expert_count = gate_proj.shape[0] // 2
    assigned = expert_ids.reshape(N_EXP, group_size * 2)
    onehot = (assigned[:, :, None] == jnp.arange(expert_count, dtype=jnp.int32)[None, None, :]).astype(jnp.int32)
    earlier_count = jnp.cumsum(onehot, axis=1) - onehot
    slot_index = jnp.sum(earlier_count * onehot, axis=2).astype(jnp.int32)
    group_index = jnp.broadcast_to(jnp.arange(N_EXP, dtype=jnp.int32)[:, None], assigned.shape)
    token_index = group_index * group_size + jnp.arange(group_size * 2, dtype=jnp.int32)[None, :] // 2
    table = jnp.full((expert_count, N_EXP, CAP), total_tokens, jnp.int32)
    table = table.at[assigned, group_index, slot_index].set(token_index.astype(jnp.int32))
    padded = jnp.concatenate([moe_tokens, jnp.zeros((1, model_width), jnp.bfloat16)], axis=0)

    def run_expert(expert):
        rows_in = padded[table[expert].reshape(-1)]
        gate_full = jnp.concatenate([gate_proj[2 * expert], gate_proj[2 * expert + 1]], axis=1)
        up_full = jnp.concatenate([up_proj[2 * expert], up_proj[2 * expert + 1]], axis=1)
        down_full = jnp.concatenate([down_proj[2 * expert], down_proj[2 * expert + 1]], axis=0)
        gate_sums = jnp.dot(rows_in, gate_full, preferred_element_type=jnp.float32)
        up_sums = jnp.dot(rows_in, up_full, preferred_element_type=jnp.float32)
        hidden = (jax.nn.silu(gate_sums) * up_sums).astype(jnp.bfloat16)
        return jnp.dot(hidden, down_full, preferred_element_type=jnp.float32)

    results = lax.map(run_expert, jnp.arange(expert_count, dtype=jnp.int32))
    results = results.reshape(expert_count, N_EXP, CAP, model_width)
    picked = results[assigned, group_index, slot_index]
    weighted = picked * route_weights.reshape(N_EXP, group_size * 2)[:, :, None]
    mixed = jnp.sum(weighted.reshape(total_tokens, 2, model_width), axis=1)
    return mixed.astype(jnp.bfloat16)


def reference(seq_inputs, step_size, write_map, read_map, decay_log, skip_gain, moe_tokens, expert_ids, route_weights, gate_proj, up_proj, down_proj):
    return (mixer_reference(seq_inputs, step_size, write_map, read_map, decay_log, skip_gain),
            expert_reference(moe_tokens, expert_ids, route_weights, gate_proj, up_proj, down_proj))
```

```python
import jax
import jax.numpy as jnp
from jax import lax
from jax.experimental import pallas as pl
from jax.experimental.pallas import tpu as pltpu
from jax.sharding import PartitionSpec as P

BLOCK = 256


HIGHEST = lax.Precision.HIGHEST


def block_chain(running, pieces):
    decay, increment = pieces
    return (decay[:, None, None] * running + increment, running)


def mixer_prepare(seq_inputs, step_size, write_map, read_map, decay_log):
    length = seq_inputs.shape[0]
    head_count = step_size.shape[0]
    state_count = write_map.shape[0]
    head_width = seq_inputs.shape[1] // head_count
    block_count = length // BLOCK
    decay_rate = -jnp.exp(decay_log)
    log_decay = (step_size * decay_rate[:, None]).reshape(head_count, block_count, BLOCK)
    order = lax.broadcasted_iota(jnp.int32, (BLOCK, BLOCK), 0)
    until = (order <= lax.broadcasted_iota(jnp.int32, (BLOCK, BLOCK), 1)).astype(jnp.float32)
    cumulative = jnp.einsum("hks,st->hkt", log_decay, until, precision=HIGHEST)
    block_ends = cumulative[:, :, BLOCK - 1]
    step_blocks = step_size.reshape(head_count, block_count, BLOCK)
    write_blocks = write_map.reshape(state_count, block_count, BLOCK)
    read_blocks = read_map.reshape(state_count, block_count, BLOCK)
    value_blocks = seq_inputs.reshape(block_count, BLOCK, head_count, head_width)
    scores = jnp.einsum(
        "nkt,nks->kts", read_blocks, write_blocks, preferred_element_type=jnp.float32
    )
    row_index = lax.broadcasted_iota(jnp.int32, (BLOCK, BLOCK), 0)
    column_index = lax.broadcasted_iota(jnp.int32, (BLOCK, BLOCK), 1)
    lower = column_index <= row_index
    difference = cumulative[:, :, :, None] - cumulative[:, :, None, :]
    decay = jnp.where(lower[None, None], jnp.exp(jnp.minimum(difference, 0.0)), 0.0)
    mixing = (scores[None] * decay * step_blocks[:, :, None, :]).astype(jnp.bfloat16)
    local_mix = jnp.einsum(
        "hkts,kshp->kthp", mixing, value_blocks, preferred_element_type=jnp.float32
    )
    weights = jnp.exp(block_ends[:, :, None] - cumulative) * step_blocks
    key_decayed = (write_blocks[None] * weights[:, None]).astype(jnp.bfloat16)
    increments = jnp.einsum(
        "hnks,kshp->khnp", key_decayed, value_blocks, preferred_element_type=jnp.float32
    )
    zero_state = jnp.zeros((head_count, state_count, head_width), jnp.float32)
    final, entering = lax.scan(block_chain, zero_state, (jnp.exp(block_ends).T, increments))
    return (local_mix, cumulative, block_ends, entering, final)


def mixer_finish(
    local_mix, cumulative, block_ends, entering, state_before, read_map, seq_inputs, skip_gain
):
    head_count = block_ends.shape[0]
    block_count = block_ends.shape[1]
    state_count = read_map.shape[0]
    head_width = entering.shape[3]
    before = jnp.cumsum(block_ends, axis=1) - block_ends
    states = jnp.exp(before).T[:, :, None, None] * state_before[None] + entering
    read_blocks = read_map.reshape(state_count, block_count, BLOCK).astype(jnp.float32)
    carried = jnp.einsum("nkt,khnp->kthp", read_blocks, states, precision=HIGHEST)
    carried = carried * jnp.exp(cumulative).transpose(1, 2, 0)[:, :, :, None]
    value_blocks = seq_inputs.reshape(block_count, BLOCK, head_count, head_width).astype(
        jnp.float32
    )
    output = local_mix + carried + skip_gain[None, None, :, None] * value_blocks
    return output.reshape(seq_inputs.shape).astype(jnp.bfloat16)


def expert_block(moe_tokens, expert_ids, route_weights, gate_proj, up_proj, down_proj):
    group_size = moe_tokens.shape[0]
    model_width = moe_tokens.shape[1]
    expert_count = lax.axis_size("exp") // 2
    capacity = min(group_size, 4 * group_size // expert_count)
    slot_count = expert_count * capacity
    assigned = expert_ids.reshape(group_size * 2)
    onehot = (
        assigned[:, None] == lax.broadcasted_iota(jnp.int32, (group_size * 2, expert_count), 1)
    ).astype(jnp.int32)
    earlier_count = jnp.cumsum(onehot, axis=0) - onehot
    position = jnp.sum((earlier_count + assigned[:, None] * capacity) * onehot, axis=1)
    matches = (
        position[:, None] == lax.broadcasted_iota(jnp.int32, (group_size * 2, slot_count), 1)
    ).astype(jnp.float32)
    dispatch = jnp.sum(matches.reshape(group_size, 2, slot_count), axis=1).astype(jnp.bfloat16)
    combine = jnp.sum(
        (matches * route_weights.reshape(group_size * 2)[:, None]).reshape(
            group_size, 2, slot_count
        ),
        axis=1,
    )
    gate_weight = gate_proj[0]
    up_weight = up_proj[0]
    down_weight = down_proj[0]
    packed = jnp.einsum(
        "is,id->sd", dispatch, moe_tokens, preferred_element_type=jnp.float32
    ).astype(jnp.bfloat16)
    doubled = jnp.broadcast_to(
        packed.reshape(expert_count, 1, capacity, model_width),
        (expert_count, 2, capacity, model_width),
    )
    arrived = lax.all_to_all(
        doubled.reshape(2 * slot_count, model_width), "exp", split_axis=0, concat_axis=0, tiled=True
    )
    gate_sums = jnp.dot(arrived, gate_weight, preferred_element_type=jnp.float32)
    up_sums = jnp.dot(arrived, up_weight, preferred_element_type=jnp.float32)
    hidden = (jax.nn.silu(gate_sums) * up_sums).astype(jnp.bfloat16)
    partial_out = jnp.dot(
        lax.all_gather(hidden, "ctx", axis=1, tiled=True),
        down_weight,
        preferred_element_type=jnp.float32,
    )
    returned = lax.all_to_all(partial_out, "exp", split_axis=0, concat_axis=0, tiled=True)
    summed = jnp.sum(returned.reshape(expert_count, 2, capacity, -1), axis=1).reshape(
        slot_count, -1
    )
    result = jnp.dot(combine, summed, precision=HIGHEST, preferred_element_type=jnp.float32)
    return result.astype(jnp.bfloat16)


MESH = pl.DeviceIdType.MESH
VMEM_BYTES = 61 * 2**20
GRID = 2
PAIR = 2
LINES = 4
CHUNKS = GRID * GRID
UNITS = 2 * CHUNKS
GROUPS = 4
F32 = jnp.float32
BF16 = jnp.bfloat16


def unit_of(t):
    return jnp.where(t == 3, 4, jnp.where(t == 4, 3, t))


def fused_kernel(
    tok_hbm,
    ids_hbm,
    route_hbm,
    seq_hbm,
    step_hbm,
    write_hbm,
    read_hbm,
    decay_ref,
    skip_ref,
    gate_hbm,
    up_hbm,
    down_hbm,
    mix_out,
    out,
    gate_w,
    up_w,
    down_w,
    tok,
    hid,
    acc,
    swap,
    ret,
    far_w,
    acc2,
    swap2,
    ret2,
    rsum,
    edge_in,
    ids,
    route,
    seq,
    step,
    write,
    read,
    local,
    grown,
    entering,
    before,
    packed,
    states,
    load_sem,
    small_sem,
    tsend,
    trecv,
    own_in_send,
    own_out_send,
    fwd_in_send,
    fwd_out_send,
    hrecv,
    wsend,
    wrecv,
    rsend,
    rrecv,
    xsend,
    xrecv,
    bsend,
    brecv,
    x2send,
    x2recv,
    b2send,
    b2recv,
    ssend,
    srecv,
):
    z = lax.axis_index("ctx")
    e = lax.axis_index("exp")
    half = lax.rem(e, PAIR)
    other = 1 - half
    px = lax.rem(e // PAIR, GRID)
    py = e // (PAIR * GRID)
    sub = tok.shape[1] // 2
    quarter = sub // 2
    part = gate_w.shape[1]
    first = part // 256 * 128
    columns = acc.shape[2]
    wide = columns // GROUPS

    end = (z == 0) | (z == LINES - 1)
    inside = (z > 0) & (z < LINES - 1)
    low = z < 2
    inner = jnp.where(low, z + 1, z - 1)
    outer = jnp.where(low, z - 1, z + 1)
    near = jnp.where(end, inner, outer)
    far = jnp.where(end, LINES - 1 - inner, inner)
    opposite = jnp.where(low, LINES - 1, 0)

    def peer(c, core):
        qx = lax.rem(px + c % GRID, GRID)
        qy = lax.rem(py + c // GRID, GRID)
        return (z, (qy * GRID + qx) * PAIR + core)

    partner = peer(0, other)
    mine = pl.ds(pl.multiple_of(half * sub, sub), sub)
    theirs = pl.ds(pl.multiple_of(other * sub, sub), sub)
    mine_a = pl.ds(pl.multiple_of(half * sub, quarter), quarter)
    mine_b = pl.ds(pl.multiple_of(half * sub + quarter, quarter), quarter)

    def remote(src, dst, ssem, rsem, device):
        return pltpu.make_async_remote_copy(
            src_ref=src,
            dst_ref=dst,
            send_sem=ssem,
            recv_sem=rsem,
            device_id=device,
            device_id_type=MESH,
        )

    left, right = pl.ds(0, first), pl.ds(first, part - first)
    loads = [
        pltpu.make_async_copy(tok_hbm.at[pl.ds(0, sub)], tok.at[0, mine], load_sem.at[0]),
        pltpu.make_async_copy(gate_hbm.at[:, left], gate_w.at[:, left], load_sem.at[1]),
        pltpu.make_async_copy(up_hbm.at[:, left], up_w.at[:, left], load_sem.at[2]),
        pltpu.make_async_copy(gate_hbm.at[:, right], gate_w.at[:, right], load_sem.at[3]),
        pltpu.make_async_copy(up_hbm.at[:, right], up_w.at[:, right], load_sem.at[4]),
        pltpu.make_async_copy(tok_hbm.at[pl.ds(sub, sub)], tok.at[1, mine], load_sem.at[5]),
        pltpu.make_async_copy(down_hbm, down_w, load_sem.at[6]),
    ]
    small = [
        pltpu.make_async_copy(src, dst, small_sem.at[i])
        for i, (src, dst) in enumerate(
            [
                (step_hbm, step),
                (write_hbm, write),
                (read_hbm, read),
                (seq_hbm, seq),
                (ids_hbm, ids),
                (route_hbm, route),
            ]
        )
    ]
    for load in loads[:6]:
        load.start()
    for load in small:
        load.start()

    barrier = pltpu.get_barrier_semaphore()
    for device in (partner, peer(1, half), peer(2, half), peer(3, half)):
        pl.semaphore_signal(barrier, inc=1, device_id=device, device_id_type=MESH)
    for j in range(LINES):

        @pl.when(z != j)
        def _():
            pl.semaphore_signal(barrier, inc=1, device_id=(j, e), device_id_type=MESH)

    pl.semaphore_wait(barrier, 4 + LINES - 1)

    def tok_rows(h):
        return tok_hbm.at[pl.ds(h * sub, sub)]

    to_partner = [
        remote(tok_rows(h), tok.at[h, mine], tsend.at[h], trecv.at[h], partner) for h in range(2)
    ]
    to_x = [
        remote(tok_rows(h), tok.at[2 + h, mine], tsend.at[2 + h], trecv.at[2 + h], peer(1, half))
        for h in range(2)
    ]
    to_y = [
        remote(tok_rows(h), tok.at[4 + h, mine], tsend.at[4 + h], trecv.at[4 + h], peer(2, half))
        for h in range(2)
    ]
    pass_x = [
        remote(
            tok.at[4 + h, mine_a], tok.at[6 + h, mine_a], tsend.at[6 + h], trecv.at[6 + h],
            peer(1, half),
        )
        for h in range(2)
    ]
    pass_y = [
        remote(
            tok.at[2 + h, mine_b], tok.at[6 + h, mine_b], tsend.at[8 + h], trecv.at[8 + h],
            peer(2, half),
        )
        for h in range(2)
    ]
    across = {
        n: remote(tok.at[n, mine], tok.at[n, mine], tsend.at[8 + n], trecv.at[8 + n], partner)
        for n in range(2, UNITS)
    }
    for h in range(2):
        to_partner[h].start()
        to_x[h].start()
        to_y[h].start()

    def lend(k):
        if k < 2:
            span = pl.ds(k * (wide // 2), wide // 2)
        else:
            span = pl.ds((k - 1) * wide, wide)
        return remote(
            down_hbm.at[opposite, :, span], far_w.at[:, span], wsend.at[k], wrecv.at[k], (inner, e)
        )

    @pl.when(end)
    def _():
        lend(0).start()

    def own_in(n):
        kind = jnp.where(end, 0, 1)
        return remote(
            hid.at[z, n], hid.at[z, n], own_in_send.at[n], hrecv.at[kind, n], (inner, e)
        )

    def own_out(n):
        return remote(hid.at[z, n], hid.at[z, n], own_out_send.at[n], hrecv.at[0, n], (outer, e))

    def fwd_in(n):
        return remote(
            hid.at[near, n], hid.at[near, n], fwd_in_send.at[n], hrecv.at[2, n], (inner, e)
        )

    def fwd_out(n):
        return remote(
            hid.at[far, n], hid.at[far, n], fwd_out_send.at[n], hrecv.at[1, n], (outer, e)
        )

    def arrived(kind, j, n):
        remote(hid.at[j, n], hid.at[j, n], own_in_send.at[n], hrecv.at[kind, n], (near, e)).wait_recv()

    def state_copy(j):
        return remote(packed, states.at[z], ssend.at[j], srecv.at[z], (j, e))

    head_count = step.shape[0]
    length = step.shape[1]
    state_count = write.shape[0]
    lanes = seq.shape[1]
    block_count = length // BLOCK
    lane_head = lax.broadcasted_iota(jnp.int32, (1, lanes), 1) // (lanes // head_count)

    def mixer_first():
        for load in small[:4]:
            load.wait()
        rows = lax.broadcasted_iota(jnp.int32, (BLOCK, BLOCK), 0)
        cols = lax.broadcasted_iota(jnp.int32, (BLOCK, BLOCK), 1)
        lower = cols <= rows
        until = (rows <= cols).astype(F32)
        since = lower.astype(F32)
        head_row = lax.broadcasted_iota(jnp.int32, (head_count, 1), 0)
        rate = jnp.zeros((head_count, 1), F32)
        for h in range(head_count):
            rate = jnp.where(head_row == h, -jnp.exp(jnp.full((head_count, 1), decay_ref[h])), rate)
        state = jnp.zeros((state_count, lanes), F32)
        gone = jnp.zeros((1, lanes), F32)
        for k in range(block_count):
            span = pl.ds(k * BLOCK, BLOCK)
            steps = step[:, span]
            log_decay = steps * rate
            cumulative = jnp.dot(
                log_decay, until, precision=HIGHEST, preferred_element_type=F32
            )
            upright = lax.dot_general(
                since,
                log_decay,
                (((1,), (1,)), ((), ())),
                precision=HIGHEST,
                preferred_element_type=F32,
            )
            block_end = cumulative[:, BLOCK - 1 :]
            weights = jnp.exp(block_end - cumulative) * steps
            keys = write[:, span]
            scores = lax.dot_general(
                read[:, span], keys, (((0,), (0,)), ((), ())), preferred_element_type=F32
            )
            values = seq[span, :]
            mixed = jnp.zeros((BLOCK, lanes), F32)
            risen = jnp.zeros((BLOCK, lanes), F32)
            increment = jnp.zeros((state_count, lanes), F32)
            ends = jnp.zeros((1, lanes), F32)
            for h in range(head_count):
                here = lane_head == h
                difference = upright[:, h : h + 1] - cumulative[h : h + 1, :]
                decay = jnp.where(lower, jnp.exp(jnp.minimum(difference, 0.0)), 0.0)
                mixing = (scores * decay * steps[h : h + 1, :]).astype(BF16)
                mixed = jnp.where(
                    here, jnp.dot(mixing, values, preferred_element_type=F32), mixed
                )
                risen = jnp.where(here, upright[:, h : h + 1], risen)
                decayed = (keys.astype(F32) * weights[h : h + 1, :]).astype(BF16)
                increment = jnp.where(
                    here, jnp.dot(decayed, values, preferred_element_type=F32), increment
                )
                ends = jnp.where(here, block_end[h : h + 1, :], ends)
            local[span, :] = mixed
            grown[span, :] = jnp.exp(risen)
            entering[k] = state
            before[k] = jnp.broadcast_to(gone, (8, lanes))
            state = jnp.exp(ends) * state + increment
            gone = gone + ends
        packed[0:state_count, :] = state
        packed[state_count:, :] = jnp.broadcast_to(gone, (8, lanes))
        states[z] = packed[...]
        for j in range(LINES):

            @pl.when(z != j)
            def _():
                state_copy(j).start()

    def mixer_second():
        for j in range(LINES):

            @pl.when(z != j)
            def _():
                remote(packed, states.at[j], ssend.at[j], srecv.at[j], (j, e)).wait_recv()

        state = jnp.zeros((state_count, lanes), F32)
        for lap in range(LINES):
            latter = states[lap]
            added = jnp.exp(latter[state_count : state_count + 1, :]) * state + latter[:state_count, :]
            state = jnp.where(lap < z, added, state)
        gain = jnp.zeros((1, lanes), F32)
        for h in range(head_count):
            gain = jnp.where(lane_head == h, skip_ref[h], gain)
        for k in range(block_count):
            span = pl.ds(k * BLOCK, BLOCK)
            full = jnp.exp(before[k][0:1, :]) * state + entering[k]
            carried = lax.dot_general(
                read[:, span].astype(F32),
                full,
                (((0,), (0,)), ((), ())),
                precision=HIGHEST,
                preferred_element_type=F32,
            )
            total = local[span, :] + carried * grown[span, :] + gain * seq[span, :].astype(F32)
            mix_out[span, :] = total.astype(mix_out.dtype)

    def share(c, h):
        qx = lax.rem(px + c % GRID, GRID)
        qy = lax.rem(py + c // GRID, GRID)
        named = ids[h * sub : (h + 1) * sub, :] == qy * GRID + qx
        return jnp.sum(jnp.where(named, route[h * sub : (h + 1) * sub, :], 0.0), axis=1, keepdims=True)

    def add_down(j, n):
        acc[n] += jnp.dot(hid[j, n], down_w[j], preferred_element_type=F32)

    def make_hidden(n, span):
        x = tok[n]
        g = jnp.dot(x, gate_w[:, span], preferred_element_type=F32)
        u = jnp.dot(x, up_w[:, span], preferred_element_type=F32)
        hid[z, n, :, span] = (jax.nn.silu(g) * u).astype(BF16)

    def tokens_ready(t):
        if t < 2:
            loads[0 if t == 0 else 5].wait()
            to_partner[t].wait_recv()
        if t == 2 or t == 4:
            h = (t - 2) // 2
            to_x[h].wait_recv()
            across[2 + h].start()
            to_y[h].wait_recv()
            across[4 + h].start()
            pass_x[h].start()
            pass_y[h].start()
            across[2 + h].wait_recv()
        if t == 3 or t == 5:
            across[4 + (t - 3) // 2].wait_recv()
        if t >= 6:
            pass_x[t - 6].wait_recv()
            pass_y[t - 6].wait_recv()
            across[t].start()
            across[t].wait_recv()

    def take_far(n):
        arrived(1, far, n)

        @pl.when(inside)
        def _():
            fwd_out(n).start()

        add_down(far, n)

    def forward_step(t, carry):
        @pl.when(t < UNITS)
        def _():
            n = unit_of(t)
            for k in range(UNITS):

                @pl.when(t == k)
                def _():
                    if k == 2:
                        mixer_first()
                    tokens_ready(k)

            @pl.when(t == 0)
            def _():
                loads[1].wait()
                loads[2].wait()

            make_hidden(n, left)

            @pl.when(t == 0)
            def _():
                loads[3].wait()
                loads[4].wait()
                loads[6].start()

            make_hidden(n, right)

            @pl.when(inside)
            def _():
                own_out(n).start()

            @pl.when(end | (t < 2))
            def _():
                own_in(n).start()

            @pl.when(t == 0)
            def _():
                loads[6].wait()

            acc[n] = jnp.dot(hid[z, n], down_w[z], preferred_element_type=F32)

        @pl.when(t >= 2)
        def _():
            n = unit_of(t - 2)
            arrived(0, near, n)

            @pl.when(inside)
            def _():
                fwd_in(n).start()

            add_down(near, n)

        @pl.when(inside & (t > 3) & (t < 6))
        def _():
            take_far(t - 4)

        @pl.when(t == UNITS - 1)
        def _():
            @pl.when(inside)
            def _():
                own_in(2).start()
                own_in(4).start()

            @pl.when(end)
            def _():
                for k in range(1, GROUPS + 1):
                    lend(k).start()

        return carry

    lax.fori_loop(0, UNITS + 2, forward_step, 0)

    @pl.when(inside)
    def _():
        for n in (3, 5, 6, 7):
            own_in(n).start()

    def exchange(n):
        return remote(acc.at[n, theirs], swap.at[n], xsend.at[n], xrecv.at[n], partner)

    def bring_home(n):
        return remote(acc.at[n, mine], ret.at[n - 2], bsend.at[n], brecv.at[n], peer(n // 2, half))

    def finish(n):
        exchange(n).wait_recv()
        acc[n, mine] += swap[n]

    def send_home(n):
        for k in range(2, UNITS):

            @pl.when(n == k)
            def _():
                bring_home(k).start()

    def exchange2(k):
        return remote(acc2.at[k, :, theirs], swap2.at[k], x2send.at[k], x2recv.at[k], partner)

    def bring_home2(k, c):
        return remote(
            acc2.at[k, pl.ds(2 * c, 2), mine],
            ret2.at[k, c - 1],
            b2send.at[k, c],
            b2recv.at[k, c],
            peer(c, half),
        )

    def edge_copy(k):
        return remote(rsum.at[k], edge_in.at[k], rsend.at[k], rrecv.at[k], (outer, e))

    def helper_dot(k):
        @pl.when(k == 0)
        def _():
            lend(0).wait_recv()
            lend(1).wait_recv()

        for i in range(1, GROUPS):

            @pl.when(k == i)
            def _():
                lend(i + 1).wait_recv()

        span = pl.ds(pl.multiple_of(k * wide, wide), wide)

        def one(n, carry):
            acc2[k, n] = jnp.dot(hid[opposite, n], far_w[:, span], preferred_element_type=F32)
            return carry

        lax.fori_loop(0, UNITS, one, 0)
        exchange2(k).start()

    def helper_home(k):
        exchange2(k).wait_recv()
        acc2[k, :, mine] += swap2[k]
        for c in range(1, CHUNKS):
            bring_home2(k, c).start()

    def helper_edge(k):
        for c in range(1, CHUNKS):
            bring_home2(k, c).wait_recv()
        for h in range(2):
            total = share(0, h) * acc2[k, h, mine]
            for c in range(1, CHUNKS):
                total += share(c, h) * ret2[k, c - 1, h]
            rsum[k, pl.ds(h * sub, sub)] = total
        edge_copy(k).start()

    def finish_step(s, carry):
        @pl.when((end & (s < UNITS)) | ((s > 1) & (s < UNITS)))
        def _():
            take_far(unit_of(s))

        @pl.when(inside & (s > 1) & (s < 4))
        def _():
            def one(i, inner_carry):
                n = unit_of((s - 2) * 4 + i)
                arrived(2, opposite, n)
                add_down(opposite, n)
                return inner_carry

            lax.fori_loop(0, 4, one, 0)

        @pl.when(s == 3)
        def _():
            for k in range(4):
                exchange(k if k < 3 else 4).start()

        @pl.when((s > 3) & (s < UNITS))
        def _():
            exchange(unit_of(s)).start()

        @pl.when(s == 4)
        def _():
            for k in range(4):
                n = k if k < 3 else 4
                finish(n)
                if n > 1:
                    bring_home(n).start()

        @pl.when((s > 4) & (s <= UNITS))
        def _():
            n = unit_of(s - 1)
            finish(n)
            send_home(n)

        @pl.when(s == 2)
        def _():
            mixer_second()

        @pl.when(inside)
        def _():
            @pl.when(((s > 2) & (s < 6)) | (s == 8))
            def _():
                helper_dot(jnp.where(s == 8, 3, s - 3))

            @pl.when(((s > 3) & (s < 7)) | (s == 9))
            def _():
                helper_home(jnp.where(s == 9, 3, s - 4))

            @pl.when(((s > 5) & (s < 9)) | (s == 10))
            def _():
                helper_edge(jnp.where(s == 10, 3, s - 6))

        return carry

    small[4].wait()
    small[5].wait()
    lax.fori_loop(0, UNITS + 3, finish_step, 0)

    for h in range(2):
        rows = pl.ds(h * sub, sub)
        total = share(0, h) * acc[h, mine]
        for c in range(1, CHUNKS):
            n = 2 * c + h
            bring_home(n).wait_recv()
            total += share(c, h) * ret[n - 2]
        swap[h] = total

    @pl.when(end)
    def _():
        for k in range(GROUPS):
            edge_copy(k).wait_recv()
            for h in range(2):
                swap[h, :, pl.ds(k * wide, wide)] += edge_in[k, pl.ds(h * sub, sub)]

    for h in range(2):
        out[pl.ds(h * sub, sub)] = swap[h].astype(out.dtype)

    for j in range(LINES):

        @pl.when(z != j)
        def _():
            state_copy(j).wait_send()

    for copy in (*to_partner, *to_x, *to_y, *pass_x, *pass_y, *across.values()):
        copy.wait_send()
    for n in range(UNITS):
        own_in(n).wait_send()
        exchange(n).wait_send()
        if n > 1:
            bring_home(n).wait_send()

    @pl.when(inside)
    def _():
        for n in range(UNITS):
            own_out(n).wait_send()
            fwd_in(n).wait_send()
            fwd_out(n).wait_send()
        for k in range(GROUPS):
            exchange2(k).wait_send()
            edge_copy(k).wait_send()
            for c in range(1, CHUNKS):
                bring_home2(k, c).wait_send()

    @pl.when(end)
    def _():
        for k in range(GROUPS + 1):
            lend(k).wait_send()


def fused(
    seq_inputs,
    step_size,
    write_map,
    read_map,
    decay_log,
    skip_gain,
    moe_tokens,
    expert_ids,
    route_weights,
    gate_proj,
    up_proj,
    down_proj,
):
    rows, width = moe_tokens.shape
    part = gate_proj.shape[2]
    columns = down_proj.shape[2]
    length, lanes = seq_inputs.shape
    state_count = write_map.shape[0]
    block_count = length // BLOCK
    sub = rows // 2
    wide = columns // GROUPS
    dma = pltpu.SemaphoreType.DMA
    vmem = pl.BlockSpec(memory_space=pltpu.VMEM)
    smem = pl.BlockSpec(memory_space=pltpu.SMEM)
    hbm = pl.BlockSpec(memory_space=pl.ANY)
    return pl.pallas_call(
        fused_kernel,
        out_shape=(
            jax.ShapeDtypeStruct(seq_inputs.shape, BF16),
            jax.ShapeDtypeStruct((rows, columns), BF16),
        ),
        in_specs=[hbm] * 7 + [smem] * 2 + [hbm] * 3,
        out_specs=(vmem, vmem),
        scratch_shapes=[
            pltpu.VMEM((width, part), BF16),
            pltpu.VMEM((width, part), BF16),
            pltpu.VMEM((LINES, part, columns), BF16),
            pltpu.VMEM((UNITS, rows, width), BF16),
            pltpu.VMEM((LINES, UNITS, rows, part), BF16),
            pltpu.VMEM((UNITS, rows, columns), F32),
            pltpu.VMEM((UNITS, sub, columns), F32),
            pltpu.VMEM((UNITS - 2, sub, columns), F32),
            pltpu.VMEM((part, columns), BF16),
            pltpu.VMEM((GROUPS, UNITS, rows, wide), F32),
            pltpu.VMEM((GROUPS, UNITS, sub, wide), F32),
            pltpu.VMEM((GROUPS, CHUNKS - 1, 2, sub, wide), F32),
            pltpu.VMEM((GROUPS, rows, wide), F32),
            pltpu.VMEM((GROUPS, rows, wide), F32),
            pltpu.VMEM(expert_ids.shape, jnp.int32),
            pltpu.VMEM(route_weights.shape, F32),
            pltpu.VMEM(seq_inputs.shape, BF16),
            pltpu.VMEM(step_size.shape, F32),
            pltpu.VMEM(write_map.shape, BF16),
            pltpu.VMEM(read_map.shape, BF16),
            pltpu.VMEM((length, lanes), F32),
            pltpu.VMEM((length, lanes), F32),
            pltpu.VMEM((block_count, state_count, lanes), F32),
            pltpu.VMEM((block_count, 8, lanes), F32),
            pltpu.VMEM((state_count + 8, lanes), F32),
            pltpu.VMEM((LINES, state_count + 8, lanes), F32),
            dma((7,)),
            dma((6,)),
            dma((16,)),
            dma((16,)),
            dma((UNITS,)),
            dma((UNITS,)),
            dma((UNITS,)),
            dma((UNITS,)),
            dma((3, UNITS)),
            dma((GROUPS + 1,)),
            dma((GROUPS + 1,)),
            dma((GROUPS,)),
            dma((GROUPS,)),
            dma((UNITS,)),
            dma((UNITS,)),
            dma((UNITS,)),
            dma((UNITS,)),
            dma((GROUPS,)),
            dma((GROUPS,)),
            dma((GROUPS, CHUNKS)),
            dma((GROUPS, CHUNKS)),
            dma((LINES,)),
            dma((LINES,)),
        ],
        compiler_params=pltpu.CompilerParams(
            collective_id=0, has_side_effects=True, vmem_limit_bytes=VMEM_BYTES
        ),
    )(
        moe_tokens,
        expert_ids,
        route_weights,
        seq_inputs,
        step_size,
        write_map,
        read_map,
        decay_log,
        skip_gain,
        gate_proj[0],
        up_proj[0],
        down_proj[0].reshape(LINES, part, columns),
    )


def fits(moe_tokens, gate_proj, down_proj):
    return (
        lax.axis_size("exp") == PAIR * GRID * GRID
        and lax.axis_size("ctx") == LINES
        and gate_proj.shape[2] % 128 == 0
        and down_proj.shape[2] % 1024 == 0
        and moe_tokens.shape[0] % 128 == 0
    )


def on_device(
    seq_inputs,
    step_size,
    write_map,
    read_map,
    decay_log,
    skip_gain,
    moe_tokens,
    expert_ids,
    route_weights,
    gate_proj,
    up_proj,
    down_proj,
):
    if fits(moe_tokens, gate_proj, down_proj):
        return fused(
            seq_inputs,
            step_size,
            write_map,
            read_map,
            decay_log,
            skip_gain,
            moe_tokens,
            expert_ids,
            route_weights,
            gate_proj,
            up_proj,
            down_proj,
        )
    local_mix, cumulative, block_ends, entering, final = mixer_prepare(
        seq_inputs, step_size, write_map, read_map, decay_log
    )
    total_log = jnp.sum(block_ends, axis=1)
    head_count, state_count, head_width = final.shape
    logs = jnp.broadcast_to(total_log[:, None, None], (head_count, 8, head_width))
    packed = jnp.concatenate([final, logs], axis=1)
    gathered = lax.all_gather(packed, "ctx")
    expert_output = expert_block(
        moe_tokens, expert_ids, route_weights, gate_proj, up_proj, down_proj
    )
    place = lax.axis_index("ctx")
    state_before = jnp.zeros_like(final)
    for lap in range(lax.axis_size("ctx")):
        latter = gathered[lap]
        decay = jnp.exp(latter[:, state_count, 0])
        added = decay[:, None, None] * state_before + latter[:, :state_count]
        state_before = jnp.where(lap < place, added, state_before)
    mixer_output = mixer_finish(
        local_mix, cumulative, block_ends, entering, state_before, read_map, seq_inputs, skip_gain
    )
    return (mixer_output, expert_output)


def solution(mesh):
    return jax.shard_map(
        on_device,
        mesh=mesh,
        in_specs=(
            P("ctx", "exp"),
            P("exp", "ctx"),
            P(None, "ctx"),
            P(None, "ctx"),
            P("exp"),
            P("exp"),
            P("exp", None),
            P("exp", None),
            P("exp", None),
            P("exp", None, "ctx"),
            P("exp", None, "ctx"),
            P("exp", None, "ctx"),
        ),
        out_specs=(P("ctx", "exp"), P("exp", "ctx")),
        check_vma=False,
    )
```

```python
import jax
import jax.numpy as jnp
from jax import lax
from jax.experimental import pallas as pl
from jax.experimental.pallas import tpu as pltpu
from jax.sharding import PartitionSpec as P

BLOCK = 256


HIGHEST = lax.Precision.HIGHEST


def block_chain(running, pieces):
    decay, increment = pieces
    return (decay[:, None, None] * running + increment, running)


def mixer_prepare(seq_inputs, step_size, write_map, read_map, decay_log):
    length = seq_inputs.shape[0]
    head_count = step_size.shape[0]
    state_count = write_map.shape[0]
    head_width = seq_inputs.shape[1] // head_count
    block_count = length // BLOCK
    decay_rate = -jnp.exp(decay_log)
    log_decay = (step_size * decay_rate[:, None]).reshape(head_count, block_count, BLOCK)
    order = lax.broadcasted_iota(jnp.int32, (BLOCK, BLOCK), 0)
    until = (order <= lax.broadcasted_iota(jnp.int32, (BLOCK, BLOCK), 1)).astype(jnp.float32)
    cumulative = jnp.einsum("hks,st->hkt", log_decay, until, precision=HIGHEST)
    block_ends = cumulative[:, :, BLOCK - 1]
    step_blocks = step_size.reshape(head_count, block_count, BLOCK)
    write_blocks = write_map.reshape(state_count, block_count, BLOCK)
    read_blocks = read_map.reshape(state_count, block_count, BLOCK)
    value_blocks = seq_inputs.reshape(block_count, BLOCK, head_count, head_width)
    scores = jnp.einsum(
        "nkt,nks->kts", read_blocks, write_blocks, preferred_element_type=jnp.float32
    )
    row_index = lax.broadcasted_iota(jnp.int32, (BLOCK, BLOCK), 0)
    column_index = lax.broadcasted_iota(jnp.int32, (BLOCK, BLOCK), 1)
    lower = column_index <= row_index
    difference = cumulative[:, :, :, None] - cumulative[:, :, None, :]
    decay = jnp.where(lower[None, None], jnp.exp(jnp.minimum(difference, 0.0)), 0.0)
    mixing = (scores[None] * decay * step_blocks[:, :, None, :]).astype(jnp.bfloat16)
    local_mix = jnp.einsum(
        "hkts,kshp->kthp", mixing, value_blocks, preferred_element_type=jnp.float32
    )
    weights = jnp.exp(block_ends[:, :, None] - cumulative) * step_blocks
    key_decayed = (write_blocks[None] * weights[:, None]).astype(jnp.bfloat16)
    increments = jnp.einsum(
        "hnks,kshp->khnp", key_decayed, value_blocks, preferred_element_type=jnp.float32
    )
    zero_state = jnp.zeros((head_count, state_count, head_width), jnp.float32)
    final, entering = lax.scan(block_chain, zero_state, (jnp.exp(block_ends).T, increments))
    return (local_mix, cumulative, block_ends, entering, final)


def mixer_finish(
    local_mix, cumulative, block_ends, entering, state_before, read_map, seq_inputs, skip_gain
):
    head_count = block_ends.shape[0]
    block_count = block_ends.shape[1]
    state_count = read_map.shape[0]
    head_width = entering.shape[3]
    before = jnp.cumsum(block_ends, axis=1) - block_ends
    states = jnp.exp(before).T[:, :, None, None] * state_before[None] + entering
    read_blocks = read_map.reshape(state_count, block_count, BLOCK).astype(jnp.float32)
    carried = jnp.einsum("nkt,khnp->kthp", read_blocks, states, precision=HIGHEST)
    carried = carried * jnp.exp(cumulative).transpose(1, 2, 0)[:, :, :, None]
    value_blocks = seq_inputs.reshape(block_count, BLOCK, head_count, head_width).astype(
        jnp.float32
    )
    output = local_mix + carried + skip_gain[None, None, :, None] * value_blocks
    return output.reshape(seq_inputs.shape).astype(jnp.bfloat16)


def expert_block(moe_tokens, expert_ids, route_weights, gate_proj, up_proj, down_proj):
    group_size = moe_tokens.shape[0]
    model_width = moe_tokens.shape[1]
    expert_count = lax.axis_size("exp") // 2
    capacity = min(group_size, 4 * group_size // expert_count)
    slot_count = expert_count * capacity
    assigned = expert_ids.reshape(group_size * 2)
    onehot = (
        assigned[:, None] == lax.broadcasted_iota(jnp.int32, (group_size * 2, expert_count), 1)
    ).astype(jnp.int32)
    earlier_count = jnp.cumsum(onehot, axis=0) - onehot
    position = jnp.sum((earlier_count + assigned[:, None] * capacity) * onehot, axis=1)
    matches = (
        position[:, None] == lax.broadcasted_iota(jnp.int32, (group_size * 2, slot_count), 1)
    ).astype(jnp.float32)
    dispatch = jnp.sum(matches.reshape(group_size, 2, slot_count), axis=1).astype(jnp.bfloat16)
    combine = jnp.sum(
        (matches * route_weights.reshape(group_size * 2)[:, None]).reshape(
            group_size, 2, slot_count
        ),
        axis=1,
    )
    gate_weight = gate_proj[0]
    up_weight = up_proj[0]
    down_weight = down_proj[0]
    packed = jnp.einsum(
        "is,id->sd", dispatch, moe_tokens, preferred_element_type=jnp.float32
    ).astype(jnp.bfloat16)
    doubled = jnp.broadcast_to(
        packed.reshape(expert_count, 1, capacity, model_width),
        (expert_count, 2, capacity, model_width),
    )
    arrived = lax.all_to_all(
        doubled.reshape(2 * slot_count, model_width), "exp", split_axis=0, concat_axis=0, tiled=True
    )
    gate_sums = jnp.dot(arrived, gate_weight, preferred_element_type=jnp.float32)
    up_sums = jnp.dot(arrived, up_weight, preferred_element_type=jnp.float32)
    hidden = (jax.nn.silu(gate_sums) * up_sums).astype(jnp.bfloat16)
    partial_out = jnp.dot(
        lax.all_gather(hidden, "ctx", axis=1, tiled=True),
        down_weight,
        preferred_element_type=jnp.float32,
    )
    returned = lax.all_to_all(partial_out, "exp", split_axis=0, concat_axis=0, tiled=True)
    summed = jnp.sum(returned.reshape(expert_count, 2, capacity, -1), axis=1).reshape(
        slot_count, -1
    )
    result = jnp.dot(combine, summed, precision=HIGHEST, preferred_element_type=jnp.float32)
    return result.astype(jnp.bfloat16)


MESH = pl.DeviceIdType.MESH
VMEM_BYTES = 58 * 2**20
GRID = 2
PAIR = 2
LINES = 4
CHUNKS = GRID * GRID
UNITS = 2 * CHUNKS
GROUPS = 8
HELPED = UNITS - 2
F32 = jnp.float32
BF16 = jnp.bfloat16


def unit_of(t):
    return jnp.where(t == 3, 4, jnp.where(t == 4, 3, t))


def fused_kernel(
    tok_hbm,
    ids_hbm,
    route_hbm,
    seq_hbm,
    step_hbm,
    write_hbm,
    read_hbm,
    decay_hbm,
    skip_hbm,
    gate_hbm,
    up_hbm,
    down_hbm,
    mix_out,
    out,
    gate_w,
    up_w,
    down_w,
    tok,
    hid,
    acc,
    swap,
    ret,
    far_w,
    acc2,
    swap2,
    ret2,
    rsum,
    edge_in,
    ids,
    route,
    share,
    decay_ref,
    skip_ref,
    seq,
    step,
    write,
    read,
    local,
    grown,
    entering,
    before,
    packed,
    states,
    load_sem,
    small_sem,
    tsend,
    trecv,
    own_in_send,
    own_out_send,
    fwd_in_send,
    fwd_out_send,
    fwd_end_send,
    hrecv,
    wsend,
    wrecv,
    rsend,
    rrecv,
    xsend,
    xrecv,
    bsend,
    brecv,
    x2send,
    x2recv,
    b2send,
    b2recv,
    ssend,
    srecv,
):
    z = lax.axis_index("ctx")
    e = lax.axis_index("exp")
    half = lax.rem(e, PAIR)
    other = 1 - half
    px = lax.rem(e // PAIR, GRID)
    py = e // (PAIR * GRID)
    rows = tok.shape[1]
    sub = rows // 2
    quarter = sub // 2
    part = gate_w.shape[1]
    first = part // 256 * 128
    columns = acc.shape[2]
    wide = columns // GROUPS

    end = (z == 0) | (z == LINES - 1)
    inside = (z > 0) & (z < LINES - 1)
    low = z < 2
    inner = jnp.where(low, z + 1, z - 1)
    outer = jnp.where(low, z - 1, z + 1)
    near = jnp.where(end, inner, outer)
    far = jnp.where(end, LINES - 1 - inner, inner)
    opposite = jnp.where(low, LINES - 1, 0)

    def peer(c, core):
        qx = lax.rem(px + c % GRID, GRID)
        qy = lax.rem(py + c // GRID, GRID)
        return (z, (qy * GRID + qx) * PAIR + core)

    partner = peer(0, other)
    mine = pl.ds(pl.multiple_of(half * sub, sub), sub)
    theirs = pl.ds(pl.multiple_of(other * sub, sub), sub)
    mine_a = pl.ds(pl.multiple_of(half * sub, quarter), quarter)
    mine_b = pl.ds(pl.multiple_of(half * sub + quarter, quarter), quarter)

    def remote(src, dst, ssem, rsem, device):
        return pltpu.make_async_remote_copy(
            src_ref=src,
            dst_ref=dst,
            send_sem=ssem,
            recv_sem=rsem,
            device_id=device,
            device_id_type=MESH,
        )

    left, right = pl.ds(0, first), pl.ds(first, part - first)
    loads = [
        pltpu.make_async_copy(tok_hbm.at[pl.ds(0, sub)], tok.at[0, mine], load_sem.at[0]),
        pltpu.make_async_copy(gate_hbm.at[:, left], gate_w.at[:, left], load_sem.at[1]),
        pltpu.make_async_copy(up_hbm.at[:, left], up_w.at[:, left], load_sem.at[2]),
        pltpu.make_async_copy(gate_hbm.at[:, right], gate_w.at[:, right], load_sem.at[3]),
        pltpu.make_async_copy(up_hbm.at[:, right], up_w.at[:, right], load_sem.at[4]),
        pltpu.make_async_copy(tok_hbm.at[pl.ds(sub, sub)], tok.at[1, mine], load_sem.at[5]),
        pltpu.make_async_copy(down_hbm, down_w, load_sem.at[6]),
    ]
    small = [
        pltpu.make_async_copy(src, dst, small_sem.at[i])
        for i, (src, dst) in enumerate(
            [
                (step_hbm, step),
                (write_hbm, write),
                (read_hbm, read),
                (seq_hbm, seq),
                (ids_hbm, ids),
                (route_hbm, route),
                (decay_hbm, decay_ref),
                (skip_hbm, skip_ref),
            ]
        )
    ]
    for load in loads[:6]:
        load.start()
    for load in small:
        load.start()

    barrier = pltpu.get_barrier_semaphore()
    for device in (partner, peer(1, half), peer(2, half), peer(3, half)):
        pl.semaphore_signal(barrier, inc=1, device_id=device, device_id_type=MESH)
    for j in range(LINES):

        @pl.when(z != j)
        def _():
            pl.semaphore_signal(barrier, inc=1, device_id=(j, e), device_id_type=MESH)

    pl.semaphore_wait(barrier, 4 + LINES - 1)

    def tok_rows(h):
        return tok_hbm.at[pl.ds(h * sub, sub)]

    to_partner = [
        remote(tok_rows(h), tok.at[h, mine], tsend.at[h], trecv.at[h], partner) for h in range(2)
    ]
    to_x = [
        remote(tok_rows(h), tok.at[2 + h, mine], tsend.at[2 + h], trecv.at[2 + h], peer(1, half))
        for h in range(2)
    ]
    to_y = [
        remote(tok_rows(h), tok.at[4 + h, mine], tsend.at[4 + h], trecv.at[4 + h], peer(2, half))
        for h in range(2)
    ]
    pass_x = [
        remote(
            tok.at[4 + h, mine_a], tok.at[6 + h, mine_a], tsend.at[6 + h], trecv.at[6 + h],
            peer(1, half),
        )
        for h in range(2)
    ]
    pass_y = [
        remote(
            tok.at[2 + h, mine_b], tok.at[6 + h, mine_b], tsend.at[8 + h], trecv.at[8 + h],
            peer(2, half),
        )
        for h in range(2)
    ]
    across = {
        n: remote(tok.at[n, mine], tok.at[n, mine], tsend.at[8 + n], trecv.at[8 + n], partner)
        for n in range(2, UNITS)
    }
    for h in range(2):
        to_partner[h].start()
        to_x[h].start()
        to_y[h].start()

    def lend(k):
        span = pl.ds(k * wide, wide)
        return remote(
            down_hbm.at[opposite, :, span], far_w.at[:, span], wsend.at[k], wrecv.at[k], (inner, e)
        )

    @pl.when(end)
    def _():
        lend(0).start()

    def own_in(n):
        kind = jnp.where(end, 0, 1)
        return remote(
            hid.at[z, n], hid.at[z, n], own_in_send.at[n], hrecv.at[kind, n], (inner, e)
        )

    def own_out(n):
        return remote(hid.at[z, n], hid.at[z, n], own_out_send.at[n], hrecv.at[0, n], (outer, e))

    def fwd_in(n):
        return remote(
            hid.at[near, n], hid.at[near, n], fwd_in_send.at[n], hrecv.at[2, n], (inner, e)
        )

    def fwd_out(n):
        return remote(
            hid.at[far, n], hid.at[far, n], fwd_out_send.at[n], hrecv.at[1, n], (outer, e)
        )

    def fwd_end(n):
        return remote(
            hid.at[opposite, n],
            hid.at[opposite, n],
            fwd_end_send.at[n - HELPED],
            hrecv.at[2, n],
            (outer, e),
        )

    def arrived(kind, j, n):
        remote(hid.at[j, n], hid.at[j, n], own_in_send.at[n], hrecv.at[kind, n], (near, e)).wait_recv()

    def state_copy(j):
        return remote(packed, states.at[z], ssend.at[j], srecv.at[z], (j, e))

    head_count = step.shape[0]
    length = step.shape[1]
    state_count = write.shape[0]
    lanes = seq.shape[1]
    block_count = length // BLOCK
    lane_head = lax.broadcasted_iota(jnp.int32, (1, lanes), 1) // (lanes // head_count)

    def mixer_first():
        for load in small:
            load.wait()
        down = lax.broadcasted_iota(jnp.int32, (BLOCK, BLOCK), 0)
        over = lax.broadcasted_iota(jnp.int32, (BLOCK, BLOCK), 1)
        lower = over <= down
        until = (down <= over).astype(F32)
        since = lower.astype(F32)
        head_row = lax.broadcasted_iota(jnp.int32, (head_count, 1), 0)
        rate = jnp.zeros((head_count, 1), F32)
        for h in range(head_count):
            rate = jnp.where(head_row == h, -jnp.exp(jnp.full((head_count, 1), decay_ref[h])), rate)
        state = jnp.zeros((state_count, lanes), F32)
        gone = jnp.zeros((1, lanes), F32)
        for k in range(block_count):
            span = pl.ds(k * BLOCK, BLOCK)
            steps = step[:, span]
            log_decay = steps * rate
            cumulative = jnp.dot(
                log_decay, until, precision=HIGHEST, preferred_element_type=F32
            )
            upright = lax.dot_general(
                since,
                log_decay,
                (((1,), (1,)), ((), ())),
                precision=HIGHEST,
                preferred_element_type=F32,
            )
            block_end = cumulative[:, BLOCK - 1 :]
            weights = jnp.exp(block_end - cumulative) * steps
            keys = write[:, span]
            scores = lax.dot_general(
                read[:, span], keys, (((0,), (0,)), ((), ())), preferred_element_type=F32
            )
            values = seq[span, :]
            mixed = jnp.zeros((BLOCK, lanes), F32)
            risen = jnp.zeros((BLOCK, lanes), F32)
            increment = jnp.zeros((state_count, lanes), F32)
            ends = jnp.zeros((1, lanes), F32)
            for h in range(head_count):
                here = lane_head == h
                difference = upright[:, h : h + 1] - cumulative[h : h + 1, :]
                decay = jnp.where(lower, jnp.exp(jnp.minimum(difference, 0.0)), 0.0)
                mixing = (scores * decay * steps[h : h + 1, :]).astype(BF16)
                mixed = jnp.where(
                    here, jnp.dot(mixing, values, preferred_element_type=F32), mixed
                )
                risen = jnp.where(here, upright[:, h : h + 1], risen)
                decayed = (keys.astype(F32) * weights[h : h + 1, :]).astype(BF16)
                increment = jnp.where(
                    here, jnp.dot(decayed, values, preferred_element_type=F32), increment
                )
                ends = jnp.where(here, block_end[h : h + 1, :], ends)
            local[span, :] = mixed
            grown[span, :] = jnp.exp(risen)
            entering[k] = state
            before[k] = jnp.broadcast_to(gone, (8, lanes))
            state = jnp.exp(ends) * state + increment
            gone = gone + ends
        packed[0:state_count, :] = state
        packed[state_count:, :] = jnp.broadcast_to(gone, (8, lanes))
        states[z] = packed[...]
        for j in range(LINES):

            @pl.when(z != j)
            def _():
                state_copy(j).start()

    def mixer_second():
        for j in range(LINES):

            @pl.when(z != j)
            def _():
                remote(packed, states.at[j], ssend.at[j], srecv.at[j], (j, e)).wait_recv()

        state = jnp.zeros((state_count, lanes), F32)
        for lap in range(LINES):
            latter = states[lap]
            added = jnp.exp(latter[state_count : state_count + 1, :]) * state + latter[:state_count, :]
            state = jnp.where(lap < z, added, state)
        gain = jnp.zeros((1, lanes), F32)
        for h in range(head_count):
            gain = jnp.where(lane_head == h, skip_ref[h], gain)
        for k in range(block_count):
            span = pl.ds(k * BLOCK, BLOCK)
            full = jnp.exp(before[k][0:1, :]) * state + entering[k]
            carried = lax.dot_general(
                read[:, span].astype(F32),
                full,
                (((0,), (0,)), ((), ())),
                precision=HIGHEST,
                preferred_element_type=F32,
            )
            total = local[span, :] + carried * grown[span, :] + gain * seq[span, :].astype(F32)
            mix_out[span, :] = total.astype(mix_out.dtype)

    def make_share():
        token = lax.broadcasted_iota(jnp.int32, (sub, rows), 1)
        place = lax.broadcasted_iota(jnp.int32, (sub, rows), 0)
        for c in range(CHUNKS):
            qx = lax.rem(px + c % GRID, GRID)
            qy = lax.rem(py + c // GRID, GRID)
            chosen = jnp.where(ids[...] == qy * GRID + qx, route[...], 0.0)
            weight = jnp.sum(chosen, axis=0, keepdims=True)
            for h in range(2):
                column = jnp.sum(
                    jnp.where(token == place + h * sub, weight, 0.0), axis=1, keepdims=True
                )
                share[2 * c + h] = jnp.broadcast_to(column, (sub, 128))

    def add_down(j, n):
        acc[n] += jnp.dot(hid[j, n], down_w[j], preferred_element_type=F32)

    def make_hidden(n, span):
        x = tok[n]
        g = jnp.dot(x, gate_w[:, span], preferred_element_type=F32)
        u = jnp.dot(x, up_w[:, span], preferred_element_type=F32)
        hid[z, n, :, span] = (jax.nn.silu(g) * u).astype(BF16)

    def tokens_ready(t):
        if t < 2:
            loads[0 if t == 0 else 5].wait()
            to_partner[t].wait_recv()
        if t == 2 or t == 4:
            h = (t - 2) // 2
            to_x[h].wait_recv()
            across[2 + h].start()
            to_y[h].wait_recv()
            across[4 + h].start()
            pass_x[h].start()
            pass_y[h].start()
            across[2 + h].wait_recv()
        if t == 3 or t == 5:
            across[4 + (t - 3) // 2].wait_recv()
        if t >= 6:
            across[t].wait_recv()

    def tokens_ahead(t):
        if t == 6 or t == 7:
            pass_x[t - 6].wait_recv()
            pass_y[t - 6].wait_recv()
            across[t].start()

    def take_far(n):
        arrived(1, far, n)

        @pl.when(inside)
        def _():
            fwd_out(n).start()

        add_down(far, n)

    def add_opposite(n):
        arrived(2, opposite, n)

        @pl.when(inside)
        def _():
            for k in range(HELPED, UNITS):

                @pl.when(n == k)
                def _():
                    fwd_end(k).start()

        add_down(opposite, n)

    def take_near(n):
        arrived(0, near, n)

        @pl.when(inside)
        def _():
            fwd_in(n).start()

        add_down(near, n)

    def own_down(t, carry):
        n = unit_of(t)
        acc[n] = jnp.dot(hid[z, n], down_w[z], preferred_element_type=F32)
        return carry

    def forward_step(t, carry):
        @pl.when(t == 2)
        def _():
            loads[6].wait()

        @pl.when((t > 1) & (t <= UNITS))
        def _():
            lax.fori_loop(jnp.where(t == 2, 0, t - 1), t, own_down, 0)

        @pl.when(t == 2)
        def _():
            mixer_first()

        @pl.when(inside & (t == 2))
        def _():
            take_near(0)
            take_far(0)

        @pl.when(t < UNITS)
        def _():
            n = unit_of(t)
            for k in range(UNITS):

                @pl.when(t == k)
                def _():
                    tokens_ready(k)

            @pl.when(t == 0)
            def _():
                loads[1].wait()
                loads[2].wait()

            make_hidden(n, left)

            @pl.when(t == 0)
            def _():
                loads[3].wait()
                loads[4].wait()
                loads[6].start()

            make_hidden(n, right)

            @pl.when(inside)
            def _():
                own_out(n).start()

            @pl.when(end | (t == 0) | (t == 2) | (t == 3))
            def _():
                own_in(n).start()

            for k in range(UNITS):

                @pl.when(t == k)
                def _():
                    tokens_ahead(k + 1)

        @pl.when(end & (t == 1))
        def _():
            lend(1).start()

        @pl.when(end & (t == UNITS - 1))
        def _():
            for k in range(2, GROUPS):
                lend(k).start()

        @pl.when(inside & (t == UNITS))
        def _():
            def one(i, inner_carry):
                add_opposite(unit_of(i))
                return inner_carry

            lax.fori_loop(0, 4, one, 0)

        @pl.when(inside & (t > 2))
        def _():
            take_near(unit_of(t - 2))

        @pl.when(inside & ((t == 4) | (t == 6)))
        def _():
            take_far(t - 2)

        return carry

    lax.fori_loop(0, UNITS + 2, forward_step, 0)

    @pl.when(inside)
    def _():
        for n in (6, 7, 3, 5, 1):
            own_in(n).start()

    def exchange(n):
        return remote(acc.at[n, theirs], swap.at[n], xsend.at[n], xrecv.at[n], partner)

    def bring_home(n):
        return remote(acc.at[n, mine], ret.at[n - 2], bsend.at[n], brecv.at[n], peer(n // 2, half))

    def finish(n):
        exchange(n).wait_recv()
        acc[n, mine] += swap[n]

    def exchange2(k):
        return remote(acc2.at[k, :, theirs], swap2.at[k], x2send.at[k], x2recv.at[k], partner)

    def bring_home2(k, c):
        return remote(
            acc2.at[k, pl.ds(2 * c, 2), mine],
            ret2.at[k, c - 1],
            b2send.at[k, c],
            b2recv.at[k, c],
            peer(c, half),
        )

    def edge_copy(k):
        return remote(rsum.at[k], edge_in.at[k], rsend.at[k], rrecv.at[k], (outer, e))

    def helper_dot(k):
        for i in range(GROUPS):

            @pl.when(k == i)
            def _():
                lend(i).wait_recv()

        span = pl.ds(pl.multiple_of(k * wide, wide), wide)
        x = hid[opposite, pl.ds(0, HELPED)].reshape(HELPED * rows, part)
        product = jnp.dot(x, far_w[:, span], preferred_element_type=F32)
        acc2[k] = product.reshape(HELPED, rows, wide)
        exchange2(k).start()

    def helper_home(k):
        exchange2(k).wait_recv()
        acc2[k, :, mine] += swap2[k]
        for c in range(1, CHUNKS - 1):
            bring_home2(k, c).start()

    def helper_edge(k):
        for c in range(1, CHUNKS - 1):
            bring_home2(k, c).wait_recv()
        for h in range(2):
            total = share[h, :, 0:1] * acc2[k, h, mine]
            for c in range(1, CHUNKS - 1):
                total += share[2 * c + h, :, 0:1] * ret2[k, c - 1, h]
            rsum[k, pl.ds(h * sub, sub)] = total
        edge_copy(k).start()

    make_share()

    @pl.when(inside)
    def _():
        def one(i, carry):
            add_opposite(unit_of(i))
            return carry

        lax.fori_loop(4, HELPED, one, 0)

    @pl.when(end)
    def _():
        def near_one(n, carry):
            take_near(n)
            return carry

        lax.fori_loop(0, UNITS, near_one, 0)

        def far_one(i, carry):
            take_far(2 * i)
            return carry

        lax.fori_loop(0, 3, far_one, 0)

    for n in (0, 2, 4):
        exchange(n).start()

    @pl.when(inside)
    def _():
        helper_dot(0)
        helper_dot(1)
        helper_home(0)

    for n in (0, 2, 4):
        finish(n)
        if n > 1:
            bring_home(n).start()

    order = (6, 7, 3, 5, 1)

    def finish_step(s, carry):
        @pl.when(s < 2)
        def _():
            add_opposite(HELPED + s)

        n = jnp.where(s < 4, HELPED + s - 2, jnp.where(s < 6, 2 * s - 5, 1))

        @pl.when((s > 1) & (s < 7))
        def _():
            take_far(n)
            exchange(n).start()

        @pl.when(inside)
        def _():
            @pl.when(s < GROUPS - 2)
            def _():
                helper_dot(s + 2)

            @pl.when(s < GROUPS - 1)
            def _():
                helper_home(s + 1)

        for i, unit in enumerate(order):

            @pl.when(s == i + 2)
            def _():
                finish(unit)
                if unit > 1:
                    bring_home(unit).start()

        @pl.when(s == 0)
        def _():
            mixer_second()

        @pl.when(inside)
        def _():
            helper_edge(s)

        return carry

    lax.fori_loop(0, GROUPS, finish_step, 0)

    for h in range(2):
        total = share[h, :, 0:1] * acc[h, mine]
        for c in range(1, CHUNKS):
            n = 2 * c + h
            bring_home(n).wait_recv()
            total += share[n, :, 0:1] * ret[n - 2]
        swap[h] = total

    @pl.when(end)
    def _():
        for k in range(GROUPS):
            edge_copy(k).wait_recv()
            for h in range(2):
                swap[h, :, pl.ds(k * wide, wide)] += edge_in[k, pl.ds(h * sub, sub)]

    for h in range(2):
        out[pl.ds(h * sub, sub)] = swap[h].astype(out.dtype)

    for j in range(LINES):

        @pl.when(z != j)
        def _():
            state_copy(j).wait_send()

    for copy in (*to_partner, *to_x, *to_y, *pass_x, *pass_y, *across.values()):
        copy.wait_send()
    for n in range(UNITS):
        own_in(n).wait_send()
        exchange(n).wait_send()
        if n > 1:
            bring_home(n).wait_send()

    @pl.when(inside)
    def _():
        for n in range(UNITS):
            own_out(n).wait_send()
            fwd_in(n).wait_send()
            fwd_out(n).wait_send()
        for k in range(GROUPS):
            exchange2(k).wait_send()
            edge_copy(k).wait_send()
            for c in range(1, CHUNKS - 1):
                bring_home2(k, c).wait_send()
        for n in range(HELPED, UNITS):
            fwd_end(n).wait_send()

    @pl.when(end)
    def _():
        for k in range(GROUPS):
            lend(k).wait_send()


def fused(
    seq_inputs,
    step_size,
    write_map,
    read_map,
    decay_log,
    skip_gain,
    moe_tokens,
    expert_ids,
    route_weights,
    gate_proj,
    up_proj,
    down_proj,
):
    rows, width = moe_tokens.shape
    part = gate_proj.shape[2]
    columns = down_proj.shape[2]
    length, lanes = seq_inputs.shape
    state_count = write_map.shape[0]
    block_count = length // BLOCK
    sub = rows // 2
    wide = columns // GROUPS
    dma = pltpu.SemaphoreType.DMA
    vmem = pl.BlockSpec(memory_space=pltpu.VMEM)
    hbm = pl.BlockSpec(memory_space=pl.ANY)
    return pl.pallas_call(
        fused_kernel,
        out_shape=(
            jax.ShapeDtypeStruct(seq_inputs.shape, BF16),
            jax.ShapeDtypeStruct((rows, columns), BF16),
        ),
        in_specs=[hbm] * 12,
        out_specs=(vmem, vmem),
        scratch_shapes=[
            pltpu.VMEM((width, part), BF16),
            pltpu.VMEM((width, part), BF16),
            pltpu.VMEM((LINES, part, columns), BF16),
            pltpu.VMEM((UNITS, rows, width), BF16),
            pltpu.VMEM((LINES, UNITS, rows, part), BF16),
            pltpu.VMEM((UNITS, rows, columns), F32),
            pltpu.VMEM((UNITS, sub, columns), F32),
            pltpu.VMEM((UNITS - 2, sub, columns), F32),
            pltpu.VMEM((part, columns), BF16),
            pltpu.VMEM((GROUPS, HELPED, rows, wide), F32),
            pltpu.VMEM((GROUPS, HELPED, sub, wide), F32),
            pltpu.VMEM((GROUPS, CHUNKS - 2, 2, sub, wide), F32),
            pltpu.VMEM((GROUPS, rows, wide), F32),
            pltpu.VMEM((GROUPS, rows, wide), F32),
            pltpu.VMEM((2, rows), jnp.int32),
            pltpu.VMEM((2, rows), F32),
            pltpu.VMEM((UNITS, sub, 128), F32),
            pltpu.SMEM(decay_log.shape, F32),
            pltpu.SMEM(skip_gain.shape, F32),
            pltpu.VMEM(seq_inputs.shape, BF16),
            pltpu.VMEM(step_size.shape, F32),
            pltpu.VMEM(write_map.shape, BF16),
            pltpu.VMEM(read_map.shape, BF16),
            pltpu.VMEM((length, lanes), F32),
            pltpu.VMEM((length, lanes), F32),
            pltpu.VMEM((block_count, state_count, lanes), F32),
            pltpu.VMEM((block_count, 8, lanes), F32),
            pltpu.VMEM((state_count + 8, lanes), F32),
            pltpu.VMEM((LINES, state_count + 8, lanes), F32),
            dma((7,)),
            dma((8,)),
            dma((16,)),
            dma((16,)),
            dma((UNITS,)),
            dma((UNITS,)),
            dma((UNITS,)),
            dma((UNITS,)),
            dma((2,)),
            dma((3, UNITS)),
            dma((GROUPS,)),
            dma((GROUPS,)),
            dma((GROUPS,)),
            dma((GROUPS,)),
            dma((UNITS,)),
            dma((UNITS,)),
            dma((UNITS,)),
            dma((UNITS,)),
            dma((GROUPS,)),
            dma((GROUPS,)),
            dma((GROUPS, CHUNKS)),
            dma((GROUPS, CHUNKS)),
            dma((LINES,)),
            dma((LINES,)),
        ],
        compiler_params=pltpu.CompilerParams(
            collective_id=0, has_side_effects=True, vmem_limit_bytes=VMEM_BYTES
        ),
    )(
        moe_tokens,
        expert_ids.T,
        route_weights.T,
        seq_inputs,
        step_size,
        write_map,
        read_map,
        decay_log,
        skip_gain,
        gate_proj[0],
        up_proj[0],
        down_proj[0].reshape(LINES, part, columns),
    )


def fits(moe_tokens, gate_proj, down_proj):
    return (
        lax.axis_size("exp") == PAIR * GRID * GRID
        and lax.axis_size("ctx") == LINES
        and gate_proj.shape[2] % 128 == 0
        and down_proj.shape[2] % 1024 == 0
        and moe_tokens.shape[0] == 128
    )


def on_device(
    seq_inputs,
    step_size,
    write_map,
    read_map,
    decay_log,
    skip_gain,
    moe_tokens,
    expert_ids,
    route_weights,
    gate_proj,
    up_proj,
    down_proj,
):
    if fits(moe_tokens, gate_proj, down_proj):
        return fused(
            seq_inputs,
            step_size,
            write_map,
            read_map,
            decay_log,
            skip_gain,
            moe_tokens,
            expert_ids,
            route_weights,
            gate_proj,
            up_proj,
            down_proj,
        )
    local_mix, cumulative, block_ends, entering, final = mixer_prepare(
        seq_inputs, step_size, write_map, read_map, decay_log
    )
    total_log = jnp.sum(block_ends, axis=1)
    head_count, state_count, head_width = final.shape
    logs = jnp.broadcast_to(total_log[:, None, None], (head_count, 8, head_width))
    packed = jnp.concatenate([final, logs], axis=1)
    gathered = lax.all_gather(packed, "ctx")
    expert_output = expert_block(
        moe_tokens, expert_ids, route_weights, gate_proj, up_proj, down_proj
    )
    place = lax.axis_index("ctx")
    state_before = jnp.zeros_like(final)
    for lap in range(lax.axis_size("ctx")):
        latter = gathered[lap]
        decay = jnp.exp(latter[:, state_count, 0])
        added = decay[:, None, None] * state_before + latter[:, :state_count]
        state_before = jnp.where(lap < place, added, state_before)
    mixer_output = mixer_finish(
        local_mix, cumulative, block_ends, entering, state_before, read_map, seq_inputs, skip_gain
    )
    return (mixer_output, expert_output)


def solution(mesh):
    return jax.shard_map(
        on_device,
        mesh=mesh,
        in_specs=(
            P("ctx", "exp"),
            P("exp", "ctx"),
            P(None, "ctx"),
            P(None, "ctx"),
            P("exp"),
            P("exp"),
            P("exp", None),
            P("exp", None),
            P("exp", None),
            P("exp", None, "ctx"),
            P("exp", None, "ctx"),
            P("exp", None, "ctx"),
        ),
        out_specs=(P("ctx", "exp"), P("exp", "ctx")),
        check_vma=False,
    )
```

```python
import jax
import jax.numpy as jnp
from jax import lax
from jax.experimental import pallas as pl
from jax.experimental.pallas import tpu as pltpu
from jax.sharding import PartitionSpec as P

BLOCK = 256


HIGHEST = lax.Precision.HIGHEST


def block_chain(running, pieces):
    decay, increment = pieces
    return (decay[:, None, None] * running + increment, running)


def mixer_prepare(seq_inputs, step_size, write_map, read_map, decay_log):
    length = seq_inputs.shape[0]
    head_count = step_size.shape[0]
    state_count = write_map.shape[0]
    head_width = seq_inputs.shape[1] // head_count
    block_count = length // BLOCK
    decay_rate = -jnp.exp(decay_log)
    log_decay = (step_size * decay_rate[:, None]).reshape(head_count, block_count, BLOCK)
    order = lax.broadcasted_iota(jnp.int32, (BLOCK, BLOCK), 0)
    until = (order <= lax.broadcasted_iota(jnp.int32, (BLOCK, BLOCK), 1)).astype(jnp.float32)
    cumulative = jnp.einsum("hks,st->hkt", log_decay, until, precision=HIGHEST)
    block_ends = cumulative[:, :, BLOCK - 1]
    step_blocks = step_size.reshape(head_count, block_count, BLOCK)
    write_blocks = write_map.reshape(state_count, block_count, BLOCK)
    read_blocks = read_map.reshape(state_count, block_count, BLOCK)
    value_blocks = seq_inputs.reshape(block_count, BLOCK, head_count, head_width)
    scores = jnp.einsum(
        "nkt,nks->kts", read_blocks, write_blocks, preferred_element_type=jnp.float32
    )
    row_index = lax.broadcasted_iota(jnp.int32, (BLOCK, BLOCK), 0)
    column_index = lax.broadcasted_iota(jnp.int32, (BLOCK, BLOCK), 1)
    lower = column_index <= row_index
    difference = cumulative[:, :, :, None] - cumulative[:, :, None, :]
    decay = jnp.where(lower[None, None], jnp.exp(jnp.minimum(difference, 0.0)), 0.0)
    mixing = (scores[None] * decay * step_blocks[:, :, None, :]).astype(jnp.bfloat16)
    local_mix = jnp.einsum(
        "hkts,kshp->kthp", mixing, value_blocks, preferred_element_type=jnp.float32
    )
    weights = jnp.exp(block_ends[:, :, None] - cumulative) * step_blocks
    key_decayed = (write_blocks[None] * weights[:, None]).astype(jnp.bfloat16)
    increments = jnp.einsum(
        "hnks,kshp->khnp", key_decayed, value_blocks, preferred_element_type=jnp.float32
    )
    zero_state = jnp.zeros((head_count, state_count, head_width), jnp.float32)
    final, entering = lax.scan(block_chain, zero_state, (jnp.exp(block_ends).T, increments))
    return (local_mix, cumulative, block_ends, entering, final)


def mixer_finish(
    local_mix, cumulative, block_ends, entering, state_before, read_map, seq_inputs, skip_gain
):
    head_count = block_ends.shape[0]
    block_count = block_ends.shape[1]
    state_count = read_map.shape[0]
    head_width = entering.shape[3]
    before = jnp.cumsum(block_ends, axis=1) - block_ends
    states = jnp.exp(before).T[:, :, None, None] * state_before[None] + entering
    read_blocks = read_map.reshape(state_count, block_count, BLOCK).astype(jnp.float32)
    carried = jnp.einsum("nkt,khnp->kthp", read_blocks, states, precision=HIGHEST)
    carried = carried * jnp.exp(cumulative).transpose(1, 2, 0)[:, :, :, None]
    value_blocks = seq_inputs.reshape(block_count, BLOCK, head_count, head_width).astype(
        jnp.float32
    )
    output = local_mix + carried + skip_gain[None, None, :, None] * value_blocks
    return output.reshape(seq_inputs.shape).astype(jnp.bfloat16)


def expert_block(moe_tokens, expert_ids, route_weights, gate_proj, up_proj, down_proj):
    group_size = moe_tokens.shape[0]
    model_width = moe_tokens.shape[1]
    expert_count = lax.axis_size("exp") // 2
    capacity = min(group_size, 4 * group_size // expert_count)
    slot_count = expert_count * capacity
    assigned = expert_ids.reshape(group_size * 2)
    onehot = (
        assigned[:, None] == lax.broadcasted_iota(jnp.int32, (group_size * 2, expert_count), 1)
    ).astype(jnp.int32)
    earlier_count = jnp.cumsum(onehot, axis=0) - onehot
    position = jnp.sum((earlier_count + assigned[:, None] * capacity) * onehot, axis=1)
    matches = (
        position[:, None] == lax.broadcasted_iota(jnp.int32, (group_size * 2, slot_count), 1)
    ).astype(jnp.float32)
    dispatch = jnp.sum(matches.reshape(group_size, 2, slot_count), axis=1).astype(jnp.bfloat16)
    combine = jnp.sum(
        (matches * route_weights.reshape(group_size * 2)[:, None]).reshape(
            group_size, 2, slot_count
        ),
        axis=1,
    )
    gate_weight = gate_proj[0]
    up_weight = up_proj[0]
    down_weight = down_proj[0]
    packed = jnp.einsum(
        "is,id->sd", dispatch, moe_tokens, preferred_element_type=jnp.float32
    ).astype(jnp.bfloat16)
    doubled = jnp.broadcast_to(
        packed.reshape(expert_count, 1, capacity, model_width),
        (expert_count, 2, capacity, model_width),
    )
    arrived = lax.all_to_all(
        doubled.reshape(2 * slot_count, model_width), "exp", split_axis=0, concat_axis=0, tiled=True
    )
    gate_sums = jnp.dot(arrived, gate_weight, preferred_element_type=jnp.float32)
    up_sums = jnp.dot(arrived, up_weight, preferred_element_type=jnp.float32)
    hidden = (jax.nn.silu(gate_sums) * up_sums).astype(jnp.bfloat16)
    partial_out = jnp.dot(
        lax.all_gather(hidden, "ctx", axis=1, tiled=True),
        down_weight,
        preferred_element_type=jnp.float32,
    )
    returned = lax.all_to_all(partial_out, "exp", split_axis=0, concat_axis=0, tiled=True)
    summed = jnp.sum(returned.reshape(expert_count, 2, capacity, -1), axis=1).reshape(
        slot_count, -1
    )
    result = jnp.dot(combine, summed, precision=HIGHEST, preferred_element_type=jnp.float32)
    return result.astype(jnp.bfloat16)


MESH = pl.DeviceIdType.MESH
VMEM_BYTES = 58 * 2**20
GRID = 2
PAIR = 2
LINES = 4
CHUNKS = GRID * GRID
UNITS = 2 * CHUNKS
GROUPS = 8
HELPED = UNITS - 2
F32 = jnp.float32
BF16 = jnp.bfloat16


def unit_of(t):
    return jnp.where(t == 3, 4, jnp.where(t == 4, 3, t))


def fused_kernel(
    tok_hbm,
    ids_hbm,
    route_hbm,
    seq_hbm,
    step_hbm,
    write_hbm,
    read_hbm,
    decay_hbm,
    skip_hbm,
    gate_hbm,
    up_hbm,
    down_hbm,
    mix_hbm,
    out_hbm,
    mix_out,
    out,
    gate_w,
    up_w,
    down_w,
    tok,
    hid,
    acc,
    swap,
    ret,
    far_w,
    acc2,
    swap2,
    ret2,
    edge,
    ids,
    route,
    share,
    decay_ref,
    skip_ref,
    seq,
    step,
    write,
    read,
    local,
    grown,
    entering,
    before,
    final,
    came,
    passed,
    load_sem,
    small_sem,
    tsend,
    trecv,
    own_in_send,
    own_out_send,
    fwd_in_send,
    fwd_out_send,
    fwd_end_send,
    hrecv,
    wsend,
    wrecv,
    rsend,
    rrecv,
    xsend,
    xrecv,
    bsend,
    brecv,
    x2send,
    x2recv,
    b2send,
    b2recv,
    ssend,
    srecv,
):
    z = lax.axis_index("ctx")
    e = lax.axis_index("exp")
    half = lax.rem(e, PAIR)
    other = 1 - half
    px = lax.rem(e // PAIR, GRID)
    py = e // (PAIR * GRID)
    rows = tok.shape[1]
    sub = rows // 2
    quarter = sub // 2
    part = gate_w.shape[1]
    first = part // 256 * 128
    columns = acc.shape[2]
    wide = columns // GROUPS

    end = (z == 0) | (z == LINES - 1)
    inside = (z > 0) & (z < LINES - 1)
    low = z < 2
    inner = jnp.where(low, z + 1, z - 1)
    outer = jnp.where(low, z - 1, z + 1)
    near = jnp.where(end, inner, outer)
    far = jnp.where(end, LINES - 1 - inner, inner)
    opposite = jnp.where(low, LINES - 1, 0)

    def peer(c, core):
        qx = lax.rem(px + c % GRID, GRID)
        qy = lax.rem(py + c // GRID, GRID)
        return (z, (qy * GRID + qx) * PAIR + core)

    partner = peer(0, other)
    mine = pl.ds(pl.multiple_of(half * sub, sub), sub)
    theirs = pl.ds(pl.multiple_of(other * sub, sub), sub)
    mine_a = pl.ds(pl.multiple_of(half * sub, quarter), quarter)
    mine_b = pl.ds(pl.multiple_of(half * sub + quarter, quarter), quarter)

    def remote(src, dst, ssem, rsem, device):
        return pltpu.make_async_remote_copy(
            src_ref=src,
            dst_ref=dst,
            send_sem=ssem,
            recv_sem=rsem,
            device_id=device,
            device_id_type=MESH,
        )

    left, right = pl.ds(0, first), pl.ds(first, part - first)
    loads = [
        pltpu.make_async_copy(tok_hbm.at[pl.ds(0, sub)], tok.at[0, mine], load_sem.at[0]),
        pltpu.make_async_copy(gate_hbm.at[:, left], gate_w.at[:, left], load_sem.at[1]),
        pltpu.make_async_copy(up_hbm.at[:, left], up_w.at[:, left], load_sem.at[2]),
        pltpu.make_async_copy(gate_hbm.at[:, right], gate_w.at[:, right], load_sem.at[3]),
        pltpu.make_async_copy(up_hbm.at[:, right], up_w.at[:, right], load_sem.at[4]),
        pltpu.make_async_copy(tok_hbm.at[pl.ds(sub, sub)], tok.at[1, mine], load_sem.at[5]),
        pltpu.make_async_copy(down_hbm, down_w, load_sem.at[6]),
    ]
    small = [
        pltpu.make_async_copy(src, dst, small_sem.at[i])
        for i, (src, dst) in enumerate(
            [
                (step_hbm, step),
                (write_hbm, write),
                (read_hbm, read),
                (seq_hbm, seq),
                (ids_hbm, ids),
                (route_hbm, route),
                (decay_hbm, decay_ref),
                (skip_hbm, skip_ref),
            ]
        )
    ]
    for load in loads[:6]:
        load.start()
    for load in small:
        load.start()

    barrier = pltpu.get_barrier_semaphore()
    for device in (partner, peer(1, half), peer(2, half), peer(3, half)):
        pl.semaphore_signal(barrier, inc=1, device_id=device, device_id_type=MESH)
    pl.semaphore_signal(barrier, inc=1, device_id=(inner, e), device_id_type=MESH)

    @pl.when(inside)
    def _():
        pl.semaphore_signal(barrier, inc=1, device_id=(outer, e), device_id_type=MESH)
        pl.semaphore_wait(barrier, 6)

    @pl.when(end)
    def _():
        pl.semaphore_wait(barrier, 5)

    def tok_rows(h):
        return tok_hbm.at[pl.ds(h * sub, sub)]

    to_partner = [
        remote(tok_rows(h), tok.at[h, mine], tsend.at[h], trecv.at[h], partner) for h in range(2)
    ]
    to_x = [
        remote(tok_rows(h), tok.at[2 + h, mine], tsend.at[2 + h], trecv.at[2 + h], peer(1, half))
        for h in range(2)
    ]
    to_y = [
        remote(tok_rows(h), tok.at[4 + h, mine], tsend.at[4 + h], trecv.at[4 + h], peer(2, half))
        for h in range(2)
    ]
    pass_x = [
        remote(
            tok.at[4 + h, mine_a], tok.at[6 + h, mine_a], tsend.at[6 + h], trecv.at[6 + h],
            peer(1, half),
        )
        for h in range(2)
    ]
    pass_y = [
        remote(
            tok.at[2 + h, mine_b], tok.at[6 + h, mine_b], tsend.at[8 + h], trecv.at[8 + h],
            peer(2, half),
        )
        for h in range(2)
    ]
    across = {
        n: remote(tok.at[n, mine], tok.at[n, mine], tsend.at[8 + n], trecv.at[8 + n], partner)
        for n in range(2, UNITS)
    }
    for h in range(2):
        to_partner[h].start()
        to_x[h].start()
        to_y[h].start()

    def lend(k, begin=0, count=part):
        span = pl.ds(k * wide, wide)
        line = pl.ds(begin, count)
        return remote(
            down_hbm.at[opposite, line, span],
            far_w.at[line, span],
            wsend.at[k],
            wrecv.at[k],
            (inner, e),
        )

    @pl.when(end)
    def _():
        lend(0, 0, part // 2).start()

    whole = pl.ds(0, part)

    def own_in(n, span=whole):
        kind = jnp.where(end, 0, 1)
        return remote(
            hid.at[z, n, :, span],
            hid.at[z, n, :, span],
            own_in_send.at[n],
            hrecv.at[kind, n],
            (inner, e),
        )

    def own_out(n, span=whole):
        return remote(
            hid.at[z, n, :, span],
            hid.at[z, n, :, span],
            own_out_send.at[n],
            hrecv.at[0, n],
            (outer, e),
        )

    def fwd_in(n):
        return remote(
            hid.at[near, n], hid.at[near, n], fwd_in_send.at[n], hrecv.at[2, n], (inner, e)
        )

    def fwd_out(n):
        return remote(
            hid.at[far, n], hid.at[far, n], fwd_out_send.at[n], hrecv.at[1, n], (outer, e)
        )

    def fwd_end(n):
        return remote(
            hid.at[opposite, n],
            hid.at[opposite, n],
            fwd_end_send.at[n - HELPED],
            hrecv.at[2, n],
            (outer, e),
        )

    def arrived(kind, j, n):
        remote(hid.at[j, n], hid.at[j, n], own_in_send.at[n], hrecv.at[kind, n], (near, e)).wait_recv()

    def state_copy():
        return remote(passed, came, ssend.at[0], srecv.at[0], (z + 1, e))

    def state_back():
        return remote(passed, came, ssend.at[0], srecv.at[0], (z - 1, e))

    head_count = step.shape[0]
    length = step.shape[1]
    state_count = write.shape[0]
    lanes = seq.shape[1]
    block_count = length // BLOCK
    lane_head = lax.broadcasted_iota(jnp.int32, (1, lanes), 1) // (lanes // head_count)

    mix_copy = pltpu.make_async_copy(mix_out, mix_hbm, load_sem.at[7])
    out_copy = pltpu.make_async_copy(out, out_hbm, load_sem.at[8])

    def mixer_first():
        for load in small:
            load.wait()
        down = lax.broadcasted_iota(jnp.int32, (BLOCK, BLOCK), 0)
        over = lax.broadcasted_iota(jnp.int32, (BLOCK, BLOCK), 1)
        lower = over <= down
        until = (down <= over).astype(F32)
        since = lower.astype(F32)
        head_row = lax.broadcasted_iota(jnp.int32, (head_count, 1), 0)
        rate = jnp.zeros((head_count, 1), F32)
        for h in range(head_count):
            rate = jnp.where(head_row == h, -jnp.exp(jnp.full((head_count, 1), decay_ref[h])), rate)
        state = jnp.zeros((state_count, lanes), F32)
        gone = jnp.zeros((1, lanes), F32)
        for k in range(block_count):
            span = pl.ds(k * BLOCK, BLOCK)
            steps = step[:, span]
            log_decay = steps * rate
            cumulative = jnp.dot(
                log_decay, until, precision=HIGHEST, preferred_element_type=F32
            )
            upright = lax.dot_general(
                since,
                log_decay,
                (((1,), (1,)), ((), ())),
                precision=HIGHEST,
                preferred_element_type=F32,
            )
            block_end = cumulative[:, BLOCK - 1 :]
            weights = jnp.exp(block_end - cumulative) * steps
            keys = write[:, span]
            scores = lax.dot_general(
                read[:, span], keys, (((0,), (0,)), ((), ())), preferred_element_type=F32
            )
            values = seq[span, :]
            mixed = jnp.zeros((BLOCK, lanes), F32)
            risen = jnp.zeros((BLOCK, lanes), F32)
            increment = jnp.zeros((state_count, lanes), F32)
            ends = jnp.zeros((1, lanes), F32)
            for h in range(head_count):
                here = lane_head == h
                difference = upright[:, h : h + 1] - cumulative[h : h + 1, :]
                decay = jnp.where(lower, jnp.exp(jnp.minimum(difference, 0.0)), 0.0)
                mixing = (scores * decay * steps[h : h + 1, :]).astype(BF16)
                mixed = jnp.where(
                    here, jnp.dot(mixing, values, preferred_element_type=F32), mixed
                )
                risen = jnp.where(here, upright[:, h : h + 1], risen)
                decayed = (keys.astype(F32) * weights[h : h + 1, :]).astype(BF16)
                increment = jnp.where(
                    here, jnp.dot(decayed, values, preferred_element_type=F32), increment
                )
                ends = jnp.where(here, block_end[h : h + 1, :], ends)
            local[span, :] = mixed
            grown[span, :] = jnp.exp(risen)
            entering[k] = state
            before[k] = jnp.broadcast_to(gone, (8, lanes))
            state = jnp.exp(ends) * state + increment
            gone = gone + ends
        final[...] = state
        before[block_count] = jnp.broadcast_to(gone, (8, lanes))

        @pl.when(z == 0)
        def _():
            came[...] = jnp.zeros((state_count, lanes), F32)
            passed[...] = state
            state_copy().start()

    def mixer_pass():
        state_back().wait_recv()
        passed[...] = jnp.exp(before[block_count][0:1, :]) * came[...] + final[...]
        state_copy().start()

    def mixer_second():
        @pl.when(z == LINES - 1)
        def _():
            state_back().wait_recv()

        state = came[...]
        gain = jnp.zeros((1, lanes), F32)
        for h in range(head_count):
            gain = jnp.where(lane_head == h, skip_ref[h], gain)
        for k in range(block_count):
            span = pl.ds(k * BLOCK, BLOCK)
            full = jnp.exp(before[k][0:1, :]) * state + entering[k]
            carried = lax.dot_general(
                read[:, span].astype(F32),
                full,
                (((0,), (0,)), ((), ())),
                precision=HIGHEST,
                preferred_element_type=F32,
            )
            total = local[span, :] + carried * grown[span, :] + gain * seq[span, :].astype(F32)
            mix_out[span, :] = total.astype(mix_out.dtype)
        mix_copy.start()

    def make_share():
        token = lax.broadcasted_iota(jnp.int32, (sub, rows), 1)
        place = lax.broadcasted_iota(jnp.int32, (sub, rows), 0)
        for c in range(CHUNKS):
            qx = lax.rem(px + c % GRID, GRID)
            qy = lax.rem(py + c // GRID, GRID)
            chosen = jnp.where(ids[...] == qy * GRID + qx, route[...], 0.0)
            weight = jnp.sum(chosen, axis=0, keepdims=True)
            for h in range(2):
                column = jnp.sum(
                    jnp.where(token == place + h * sub, weight, 0.0), axis=1, keepdims=True
                )
                share[2 * c + h] = jnp.broadcast_to(column, (sub, 128))

    def add_down(j, n):
        acc[n] += jnp.dot(hid[j, n], down_w[j], preferred_element_type=F32)

    def make_hidden(n, span):
        x = tok[n]
        g = jnp.dot(x, gate_w[:, span], preferred_element_type=F32)
        u = jnp.dot(x, up_w[:, span], preferred_element_type=F32)
        hid[z, n, :, span] = (jax.nn.silu(g) * u).astype(BF16)

    def tokens_ready(t):
        if t < 2:
            loads[0 if t == 0 else 5].wait()
            to_partner[t].wait_recv()
        if t == 2 or t == 4:
            h = (t - 2) // 2
            to_x[h].wait_recv()
            across[2 + h].start()
            to_y[h].wait_recv()
            across[4 + h].start()
            pass_x[h].start()
            pass_y[h].start()
            across[2 + h].wait_recv()
        if t == 3 or t == 5:
            across[4 + (t - 3) // 2].wait_recv()
        if t >= 6:
            across[t].wait_recv()

    def tokens_ahead(t):
        if t == 6 or t == 7:
            pass_x[t - 6].wait_recv()
            pass_y[t - 6].wait_recv()
            across[t].start()

    def take_far(n):
        arrived(1, far, n)

        @pl.when(inside)
        def _():
            fwd_out(n).start()

        add_down(far, n)

    def add_opposite(n):
        arrived(2, opposite, n)

        @pl.when(inside)
        def _():
            for k in range(HELPED, UNITS):

                @pl.when(n == k)
                def _():
                    fwd_end(k).start()

        add_down(opposite, n)

    def take_near(n):
        arrived(0, near, n)

        @pl.when(inside)
        def _():
            fwd_in(n).start()

        add_down(near, n)

    def own_down(t, carry):
        n = unit_of(t)
        acc[n] = jnp.dot(hid[z, n], down_w[z], preferred_element_type=F32)
        return carry

    def exchange(n):
        return remote(acc.at[n, theirs], swap.at[n], xsend.at[n], xrecv.at[n], partner)

    def bring_home(n):
        return remote(acc.at[n, mine], ret.at[n - 2], bsend.at[n], brecv.at[n], peer(n // 2, half))

    def finish(n):
        exchange(n).wait_recv()
        acc[n, mine] += swap[n]

    def early_finish():
        for n in (0, 2, 4):
            finish(n)
            if n > 1:
                bring_home(n).start()

    def forward_step(t, carry):
        @pl.when(t == 2)
        def _():
            loads[6].wait()

        @pl.when((t > 1) & (t <= UNITS))
        def _():
            lax.fori_loop(jnp.where(t == 2, 0, t - 1), t, own_down, 0)

        @pl.when(t == 2)
        def _():
            mixer_first()

        @pl.when(((z == 1) & (t == 4)) | ((z == 2) & (t == 6)))
        def _():
            mixer_pass()

        @pl.when(inside & (t == 2))
        def _():
            take_near(0)
            take_far(0)

        @pl.when(t < UNITS)
        def _():
            n = unit_of(t)
            for k in range(UNITS):

                @pl.when(t == k)
                def _():
                    tokens_ready(k)
                    if k == 2:

                        @pl.when(inside)
                        def _():
                            take_near(1)

            @pl.when(t == 0)
            def _():
                loads[1].wait()
                loads[2].wait()

            make_hidden(n, left)

            @pl.when(t == 0)
            def _():
                own_in(0, left).start()

                @pl.when(inside)
                def _():
                    own_out(0, left).start()

                loads[3].wait()
                loads[4].wait()
                loads[6].start()

            make_hidden(n, right)

            @pl.when(t == 0)
            def _():
                own_in(0, right).start()

                @pl.when(inside)
                def _():
                    own_out(0, right).start()

            @pl.when(inside & (t > 0))
            def _():
                own_out(n).start()

            @pl.when((end & (t > 0)) | (t == 2) | (t == 3))
            def _():
                own_in(n).start()

            for k in range(UNITS):

                @pl.when(t == k)
                def _():
                    tokens_ahead(k + 1)

        @pl.when(end & (t == 1))
        def _():
            lend(0, part // 2, part - part // 2).start()

        @pl.when(end & (t == UNITS - 1))
        def _():
            for k in range(1, GROUPS):
                lend(k).start()

        @pl.when(inside & (t == UNITS))
        def _():
            def one(i, inner_carry):
                add_opposite(unit_of(i))
                return inner_carry

            lax.fori_loop(0, 4, one, 0)
            for n in (0, 2, 4):
                exchange(n).start()

        @pl.when(inside & (t == UNITS + 1))
        def _():
            early_finish()

        @pl.when(inside & (t > 3))
        def _():
            take_near(unit_of(t - 2))

        @pl.when(inside & ((t == 4) | (t == 6)))
        def _():
            take_far(t - 2)

        return carry

    lax.fori_loop(0, UNITS + 2, forward_step, 0)

    @pl.when(inside)
    def _():
        for n in (6, 7, 3, 5, 1):
            own_in(n).start()

    def exchange2(k):
        return remote(acc2.at[k, :, theirs], swap2.at[k], x2send.at[k], x2recv.at[k], partner)

    def bring_home2(k, c):
        return remote(
            acc2.at[k, pl.ds(2 * c, 2), mine],
            ret2.at[k, c - 1],
            b2send.at[k, c],
            b2recv.at[k, c],
            peer(c, half),
        )

    def edge_copy(k):
        return remote(edge.at[k], edge.at[k], rsend.at[k], rrecv.at[k], (outer, e))

    def helper_dot(k):
        for i in range(GROUPS):

            @pl.when(k == i)
            def _():
                lend(i).wait_recv()

        span = pl.ds(pl.multiple_of(k * wide, wide), wide)
        x = hid[opposite, pl.ds(0, HELPED)].reshape(HELPED * rows, part)
        product = jnp.dot(x, far_w[:, span], preferred_element_type=F32)
        acc2[k] = product.reshape(HELPED, rows, wide)
        exchange2(k).start()

    def helper_home(k):
        exchange2(k).wait_recv()
        acc2[k, :, mine] += swap2[k]
        for c in range(1, CHUNKS - 1):
            bring_home2(k, c).start()

    def helper_edge(k):
        for c in range(1, CHUNKS - 1):
            bring_home2(k, c).wait_recv()
        for h in range(2):
            total = share[h, :, 0:1] * acc2[k, h, mine]
            for c in range(1, CHUNKS - 1):
                total += share[2 * c + h, :, 0:1] * ret2[k, c - 1, h]
            edge[k, pl.ds(h * sub, sub)] = total.astype(edge.dtype)
        edge_copy(k).start()

    make_share()

    @pl.when(inside)
    def _():
        def one(i, carry):
            add_opposite(unit_of(i))
            return carry

        lax.fori_loop(4, HELPED, one, 0)

    @pl.when(end)
    def _():
        def near_one(n, carry):
            take_near(n)
            return carry

        lax.fori_loop(0, UNITS, near_one, 0)

        def far_one(i, carry):
            take_far(2 * i)
            return carry

        lax.fori_loop(0, 3, far_one, 0)
        for n in (0, 2, 4):
            exchange(n).start()
        early_finish()

    @pl.when(inside)
    def _():
        add_opposite(HELPED)
        helper_dot(0)
        helper_dot(1)
        helper_home(0)

    order = (6, 7, 3, 5, 1)
    home = (2, 4, 6, 6)

    def finish_step(s, carry):
        @pl.when((s == 1) | (end & (s == 0)))
        def _():
            add_opposite(HELPED + s)

        n = jnp.where(s < 4, HELPED + s - 2, jnp.where(s < 6, 2 * s - 5, 1))

        @pl.when((s > 1) & (s < 7))
        def _():
            take_far(n)
            exchange(n).start()

        @pl.when(inside)
        def _():
            @pl.when(s < 6)
            def _():
                helper_dot(s + 2)

            @pl.when(s < 7)
            def _():
                helper_home(s + 1)

        for i, unit in enumerate(order):

            @pl.when(s == i + 2)
            def _():
                finish(unit)

            if unit > 1:

                @pl.when(s == jnp.where(inside, home[i], i + 2))
                def _():
                    bring_home(unit).start()

        @pl.when(s == 0)
        def _():
            mixer_second()

        @pl.when(inside & (s > 6))
        def _():
            helper_edge(s - 7)

        return carry

    lax.fori_loop(0, GROUPS + 7, finish_step, 0)

    for h in range(2):
        total = share[h, :, 0:1] * acc[h, mine]
        for c in range(1, CHUNKS):
            n = 2 * c + h
            bring_home(n).wait_recv()
            total += share[n, :, 0:1] * ret[n - 2]
        swap[h] = total

    @pl.when(end)
    def _():
        for k in range(GROUPS):
            edge_copy(k).wait_recv()
            span = pl.ds(k * wide, wide)
            for h in range(2):
                line = pl.ds(h * sub, sub)
                out[line, span] = (swap[h, :, span] + edge[k, line].astype(F32)).astype(out.dtype)

    @pl.when(inside)
    def _():
        for h in range(2):
            out[pl.ds(h * sub, sub)] = swap[h].astype(out.dtype)

    out_copy.start()
    @pl.when(z < LINES - 1)
    def _():
        state_copy().wait_send()

    for copy in (*to_partner, *to_x, *to_y, *pass_x, *pass_y, *across.values()):
        copy.wait_send()
    for n in range(UNITS):
        own_in(n).wait_send()
        exchange(n).wait_send()
        if n > 1:
            bring_home(n).wait_send()

    @pl.when(inside)
    def _():
        for n in range(UNITS):
            own_out(n).wait_send()
            fwd_in(n).wait_send()
            fwd_out(n).wait_send()
        for k in range(GROUPS):
            exchange2(k).wait_send()
            edge_copy(k).wait_send()
            for c in range(1, CHUNKS - 1):
                bring_home2(k, c).wait_send()
        for n in range(HELPED, UNITS):
            fwd_end(n).wait_send()

    @pl.when(end)
    def _():
        for k in range(GROUPS):
            lend(k).wait_send()

    mix_copy.wait()
    out_copy.wait()


def fused(
    seq_inputs,
    step_size,
    write_map,
    read_map,
    decay_log,
    skip_gain,
    moe_tokens,
    expert_ids,
    route_weights,
    gate_proj,
    up_proj,
    down_proj,
):
    rows, width = moe_tokens.shape
    part = gate_proj.shape[2]
    columns = down_proj.shape[2]
    length, lanes = seq_inputs.shape
    state_count = write_map.shape[0]
    block_count = length // BLOCK
    sub = rows // 2
    wide = columns // GROUPS
    dma = pltpu.SemaphoreType.DMA
    hbm = pl.BlockSpec(memory_space=pl.ANY)
    results = pl.pallas_call(
        fused_kernel,
        out_shape=(
            jax.ShapeDtypeStruct(seq_inputs.shape, BF16),
            jax.ShapeDtypeStruct((rows, columns), BF16),
        ),
        in_specs=[hbm] * 12,
        out_specs=(hbm, hbm),
        scratch_shapes=[
            pltpu.VMEM(seq_inputs.shape, BF16),
            pltpu.VMEM((rows, columns), BF16),
            pltpu.VMEM((width, part), BF16),
            pltpu.VMEM((width, part), BF16),
            pltpu.VMEM((LINES, part, columns), BF16),
            pltpu.VMEM((UNITS, rows, width), BF16),
            pltpu.VMEM((LINES, UNITS, rows, part), BF16),
            pltpu.VMEM((UNITS, rows, columns), F32),
            pltpu.VMEM((UNITS, sub, columns), F32),
            pltpu.VMEM((UNITS - 2, sub, columns), F32),
            pltpu.VMEM((part, columns), BF16),
            pltpu.VMEM((GROUPS, HELPED, rows, wide), F32),
            pltpu.VMEM((GROUPS, HELPED, sub, wide), F32),
            pltpu.VMEM((GROUPS, CHUNKS - 2, 2, sub, wide), F32),
            pltpu.VMEM((GROUPS, rows, wide), BF16),
            pltpu.VMEM((2, rows), jnp.int32),
            pltpu.VMEM((2, rows), F32),
            pltpu.VMEM((UNITS, sub, 128), F32),
            pltpu.SMEM(decay_log.shape, F32),
            pltpu.SMEM(skip_gain.shape, F32),
            pltpu.VMEM(seq_inputs.shape, BF16),
            pltpu.VMEM(step_size.shape, F32),
            pltpu.VMEM(write_map.shape, BF16),
            pltpu.VMEM(read_map.shape, BF16),
            pltpu.VMEM((length, lanes), F32),
            pltpu.VMEM((length, lanes), F32),
            pltpu.VMEM((block_count, state_count, lanes), F32),
            pltpu.VMEM((block_count + 1, 8, lanes), F32),
            pltpu.VMEM((state_count, lanes), F32),
            pltpu.VMEM((state_count, lanes), F32),
            pltpu.VMEM((state_count, lanes), F32),
            dma((9,)),
            dma((8,)),
            dma((16,)),
            dma((16,)),
            dma((UNITS,)),
            dma((UNITS,)),
            dma((UNITS,)),
            dma((UNITS,)),
            dma((2,)),
            dma((3, UNITS)),
            dma((GROUPS,)),
            dma((GROUPS,)),
            dma((GROUPS,)),
            dma((GROUPS,)),
            dma((UNITS,)),
            dma((UNITS,)),
            dma((UNITS,)),
            dma((UNITS,)),
            dma((GROUPS,)),
            dma((GROUPS,)),
            dma((GROUPS, CHUNKS)),
            dma((GROUPS, CHUNKS)),
            dma((1,)),
            dma((1,)),
        ],
        compiler_params=pltpu.CompilerParams(
            collective_id=0, has_side_effects=True, vmem_limit_bytes=VMEM_BYTES
        ),
    )(
        moe_tokens,
        expert_ids.T,
        route_weights.T,
        seq_inputs,
        step_size,
        write_map,
        read_map,
        decay_log,
        skip_gain,
        gate_proj[0],
        up_proj[0],
        down_proj[0].reshape(LINES, part, columns),
    )
    return hand_over(*results)


def hand_over_kernel(*refs):
    count = (len(refs) - 2) // 3
    sources, targets, held = refs[:count], refs[count : 2 * count], refs[2 * count : 3 * count]
    in_sem, out_sem = refs[3 * count :]
    pieces = in_sem.shape[1]
    loads, stores = [], []
    for i in range(count):
        step = held[i].shape[0] // pieces
        for k in range(pieces):
            line = pl.ds(k * step, step)
            loads.append(
                pltpu.make_async_copy(sources[i].at[line], held[i].at[line], in_sem.at[i, k])
            )
            stores.append(
                pltpu.make_async_copy(held[i].at[line], targets[i].at[line], out_sem.at[i, k])
            )
    for load in loads:
        load.start()
    for load, store in zip(loads, stores):
        load.wait()
        store.start()
    for store in stores:
        store.wait()


def hand_over(*arrays):
    hbm = pl.BlockSpec(memory_space=pltpu.HBM)
    pieces = 2
    dma = pltpu.SemaphoreType.DMA((len(arrays), pieces))
    return pl.pallas_call(
        hand_over_kernel,
        out_shape=tuple(jax.ShapeDtypeStruct(a.shape, a.dtype) for a in arrays),
        in_specs=[hbm] * len(arrays),
        out_specs=(hbm,) * len(arrays),
        scratch_shapes=[pltpu.VMEM(a.shape, a.dtype) for a in arrays] + [dma, dma],
        compiler_params=pltpu.CompilerParams(vmem_limit_bytes=VMEM_BYTES),
    )(*arrays)


def fits(moe_tokens, gate_proj, down_proj):
    return (
        lax.axis_size("exp") == PAIR * GRID * GRID
        and lax.axis_size("ctx") == LINES
        and gate_proj.shape[2] % 128 == 0
        and down_proj.shape[2] % 1024 == 0
        and moe_tokens.shape[0] == 128
    )


def on_device(
    seq_inputs,
    step_size,
    write_map,
    read_map,
    decay_log,
    skip_gain,
    moe_tokens,
    expert_ids,
    route_weights,
    gate_proj,
    up_proj,
    down_proj,
):
    if fits(moe_tokens, gate_proj, down_proj):
        return fused(
            seq_inputs,
            step_size,
            write_map,
            read_map,
            decay_log,
            skip_gain,
            moe_tokens,
            expert_ids,
            route_weights,
            gate_proj,
            up_proj,
            down_proj,
        )
    local_mix, cumulative, block_ends, entering, final = mixer_prepare(
        seq_inputs, step_size, write_map, read_map, decay_log
    )
    total_log = jnp.sum(block_ends, axis=1)
    head_count, state_count, head_width = final.shape
    logs = jnp.broadcast_to(total_log[:, None, None], (head_count, 8, head_width))
    packed = jnp.concatenate([final, logs], axis=1)
    gathered = lax.all_gather(packed, "ctx")
    expert_output = expert_block(
        moe_tokens, expert_ids, route_weights, gate_proj, up_proj, down_proj
    )
    place = lax.axis_index("ctx")
    state_before = jnp.zeros_like(final)
    for lap in range(lax.axis_size("ctx")):
        latter = gathered[lap]
        decay = jnp.exp(latter[:, state_count, 0])
        added = decay[:, None, None] * state_before + latter[:, :state_count]
        state_before = jnp.where(lap < place, added, state_before)
    mixer_output = mixer_finish(
        local_mix, cumulative, block_ends, entering, state_before, read_map, seq_inputs, skip_gain
    )
    return (mixer_output, expert_output)


def solution(mesh):
    return jax.shard_map(
        on_device,
        mesh=mesh,
        in_specs=(
            P("ctx", "exp"),
            P("exp", "ctx"),
            P(None, "ctx"),
            P(None, "ctx"),
            P("exp"),
            P("exp"),
            P("exp", None),
            P("exp", None),
            P("exp", None),
            P("exp", None, "ctx"),
            P("exp", None, "ctx"),
            P("exp", None, "ctx"),
        ),
        out_specs=(P("ctx", "exp"), P("exp", "ctx")),
        check_vma=False,
    )
```

```python
import jax
import jax.numpy as jnp
from jax import lax
from jax.experimental import pallas as pl
from jax.experimental.pallas import tpu as pltpu
from jax.sharding import PartitionSpec as P

BLOCK = 256


HIGHEST = lax.Precision.HIGHEST


def block_chain(running, pieces):
    decay, increment = pieces
    return (decay[:, None, None] * running + increment, running)


def mixer_prepare(seq_inputs, step_size, write_map, read_map, decay_log):
    length = seq_inputs.shape[0]
    head_count = step_size.shape[0]
    state_count = write_map.shape[0]
    head_width = seq_inputs.shape[1] // head_count
    block_count = length // BLOCK
    decay_rate = -jnp.exp(decay_log)
    log_decay = (step_size * decay_rate[:, None]).reshape(head_count, block_count, BLOCK)
    order = lax.broadcasted_iota(jnp.int32, (BLOCK, BLOCK), 0)
    until = (order <= lax.broadcasted_iota(jnp.int32, (BLOCK, BLOCK), 1)).astype(jnp.float32)
    cumulative = jnp.einsum("hks,st->hkt", log_decay, until, precision=HIGHEST)
    block_ends = cumulative[:, :, BLOCK - 1]
    step_blocks = step_size.reshape(head_count, block_count, BLOCK)
    write_blocks = write_map.reshape(state_count, block_count, BLOCK)
    read_blocks = read_map.reshape(state_count, block_count, BLOCK)
    value_blocks = seq_inputs.reshape(block_count, BLOCK, head_count, head_width)
    scores = jnp.einsum(
        "nkt,nks->kts", read_blocks, write_blocks, preferred_element_type=jnp.float32
    )
    row_index = lax.broadcasted_iota(jnp.int32, (BLOCK, BLOCK), 0)
    column_index = lax.broadcasted_iota(jnp.int32, (BLOCK, BLOCK), 1)
    lower = column_index <= row_index
    difference = cumulative[:, :, :, None] - cumulative[:, :, None, :]
    decay = jnp.where(lower[None, None], jnp.exp(jnp.minimum(difference, 0.0)), 0.0)
    mixing = (scores[None] * decay * step_blocks[:, :, None, :]).astype(jnp.bfloat16)
    local_mix = jnp.einsum(
        "hkts,kshp->kthp", mixing, value_blocks, preferred_element_type=jnp.float32
    )
    weights = jnp.exp(block_ends[:, :, None] - cumulative) * step_blocks
    key_decayed = (write_blocks[None] * weights[:, None]).astype(jnp.bfloat16)
    increments = jnp.einsum(
        "hnks,kshp->khnp", key_decayed, value_blocks, preferred_element_type=jnp.float32
    )
    zero_state = jnp.zeros((head_count, state_count, head_width), jnp.float32)
    final, entering = lax.scan(block_chain, zero_state, (jnp.exp(block_ends).T, increments))
    return (local_mix, cumulative, block_ends, entering, final)


def mixer_finish(
    local_mix, cumulative, block_ends, entering, state_before, read_map, seq_inputs, skip_gain
):
    head_count = block_ends.shape[0]
    block_count = block_ends.shape[1]
    state_count = read_map.shape[0]
    head_width = entering.shape[3]
    before = jnp.cumsum(block_ends, axis=1) - block_ends
    states = jnp.exp(before).T[:, :, None, None] * state_before[None] + entering
    read_blocks = read_map.reshape(state_count, block_count, BLOCK).astype(jnp.float32)
    carried = jnp.einsum("nkt,khnp->kthp", read_blocks, states, precision=HIGHEST)
    carried = carried * jnp.exp(cumulative).transpose(1, 2, 0)[:, :, :, None]
    value_blocks = seq_inputs.reshape(block_count, BLOCK, head_count, head_width).astype(
        jnp.float32
    )
    output = local_mix + carried + skip_gain[None, None, :, None] * value_blocks
    return output.reshape(seq_inputs.shape).astype(jnp.bfloat16)


def expert_block(moe_tokens, expert_ids, route_weights, gate_proj, up_proj, down_proj):
    group_size = moe_tokens.shape[0]
    model_width = moe_tokens.shape[1]
    expert_count = lax.axis_size("exp") // 2
    capacity = min(group_size, 4 * group_size // expert_count)
    slot_count = expert_count * capacity
    assigned = expert_ids.reshape(group_size * 2)
    onehot = (
        assigned[:, None] == lax.broadcasted_iota(jnp.int32, (group_size * 2, expert_count), 1)
    ).astype(jnp.int32)
    earlier_count = jnp.cumsum(onehot, axis=0) - onehot
    position = jnp.sum((earlier_count + assigned[:, None] * capacity) * onehot, axis=1)
    matches = (
        position[:, None] == lax.broadcasted_iota(jnp.int32, (group_size * 2, slot_count), 1)
    ).astype(jnp.float32)
    dispatch = jnp.sum(matches.reshape(group_size, 2, slot_count), axis=1).astype(jnp.bfloat16)
    combine = jnp.sum(
        (matches * route_weights.reshape(group_size * 2)[:, None]).reshape(
            group_size, 2, slot_count
        ),
        axis=1,
    )
    gate_weight = gate_proj[0]
    up_weight = up_proj[0]
    down_weight = down_proj[0]
    packed = jnp.einsum(
        "is,id->sd", dispatch, moe_tokens, preferred_element_type=jnp.float32
    ).astype(jnp.bfloat16)
    doubled = jnp.broadcast_to(
        packed.reshape(expert_count, 1, capacity, model_width),
        (expert_count, 2, capacity, model_width),
    )
    arrived = lax.all_to_all(
        doubled.reshape(2 * slot_count, model_width), "exp", split_axis=0, concat_axis=0, tiled=True
    )
    gate_sums = jnp.dot(arrived, gate_weight, preferred_element_type=jnp.float32)
    up_sums = jnp.dot(arrived, up_weight, preferred_element_type=jnp.float32)
    hidden = (jax.nn.silu(gate_sums) * up_sums).astype(jnp.bfloat16)
    partial_out = jnp.dot(
        lax.all_gather(hidden, "ctx", axis=1, tiled=True),
        down_weight,
        preferred_element_type=jnp.float32,
    )
    returned = lax.all_to_all(partial_out, "exp", split_axis=0, concat_axis=0, tiled=True)
    summed = jnp.sum(returned.reshape(expert_count, 2, capacity, -1), axis=1).reshape(
        slot_count, -1
    )
    result = jnp.dot(combine, summed, precision=HIGHEST, preferred_element_type=jnp.float32)
    return result.astype(jnp.bfloat16)


MESH = pl.DeviceIdType.MESH
VMEM_BYTES = 58 * 2**20
GRID = 2
PAIR = 2
LINES = 4
CHUNKS = GRID * GRID
UNITS = 2 * CHUNKS
GROUPS = 8
HELPED = UNITS - 2
F32 = jnp.float32
BF16 = jnp.bfloat16


def unit_of(t):
    return jnp.where(t == 3, 4, jnp.where(t == 4, 3, t))


def fused_kernel(
    tok_hbm,
    ids_hbm,
    route_hbm,
    seq_hbm,
    step_hbm,
    write_hbm,
    read_hbm,
    decay_hbm,
    skip_hbm,
    gate_hbm,
    up_hbm,
    down_hbm,
    mix_hbm,
    out_hbm,
    mix_out,
    out,
    gate_w,
    up_w,
    down_w,
    tok,
    hid,
    acc,
    swap,
    ret,
    far_w,
    acc2,
    swap2,
    ret2,
    edge,
    ids,
    route,
    share,
    decay_ref,
    skip_ref,
    seq,
    step,
    write,
    read,
    local,
    grown,
    entering,
    before,
    final,
    came,
    passed,
    load_sem,
    small_sem,
    tsend,
    trecv,
    own_in_send,
    own_out_send,
    fwd_in_send,
    fwd_out_send,
    fwd_end_send,
    hrecv,
    wsend,
    wrecv,
    rsend,
    rrecv,
    xsend,
    xrecv,
    bsend,
    brecv,
    x2send,
    x2recv,
    b2send,
    b2recv,
    ssend,
    srecv,
):
    z = lax.axis_index("ctx")
    e = lax.axis_index("exp")
    half = lax.rem(e, PAIR)
    other = 1 - half
    px = lax.rem(e // PAIR, GRID)
    py = e // (PAIR * GRID)
    rows = tok.shape[1]
    sub = rows // 2
    quarter = sub // 2
    part = gate_w.shape[1]
    first = part // 256 * 128
    columns = acc.shape[2]
    wide = columns // GROUPS

    end = (z == 0) | (z == LINES - 1)
    inside = (z > 0) & (z < LINES - 1)
    low = z < 2
    inner = jnp.where(low, z + 1, z - 1)
    outer = jnp.where(low, z - 1, z + 1)
    near = jnp.where(end, inner, outer)
    far = jnp.where(end, LINES - 1 - inner, inner)
    opposite = jnp.where(low, LINES - 1, 0)

    def peer(c, core):
        qx = lax.rem(px + c % GRID, GRID)
        qy = lax.rem(py + c // GRID, GRID)
        return (z, (qy * GRID + qx) * PAIR + core)

    partner = peer(0, other)
    mine = pl.ds(pl.multiple_of(half * sub, sub), sub)
    theirs = pl.ds(pl.multiple_of(other * sub, sub), sub)
    mine_a = pl.ds(pl.multiple_of(half * sub, quarter), quarter)
    mine_b = pl.ds(pl.multiple_of(half * sub + quarter, quarter), quarter)

    def remote(src, dst, ssem, rsem, device):
        return pltpu.make_async_remote_copy(
            src_ref=src,
            dst_ref=dst,
            send_sem=ssem,
            recv_sem=rsem,
            device_id=device,
            device_id_type=MESH,
        )

    left, right = pl.ds(0, first), pl.ds(first, part - first)
    loads = [
        pltpu.make_async_copy(tok_hbm.at[pl.ds(0, sub)], tok.at[0, mine], load_sem.at[0]),
        pltpu.make_async_copy(gate_hbm.at[:, left], gate_w.at[:, left], load_sem.at[1]),
        pltpu.make_async_copy(up_hbm.at[:, left], up_w.at[:, left], load_sem.at[2]),
        pltpu.make_async_copy(gate_hbm.at[:, right], gate_w.at[:, right], load_sem.at[3]),
        pltpu.make_async_copy(up_hbm.at[:, right], up_w.at[:, right], load_sem.at[4]),
        pltpu.make_async_copy(tok_hbm.at[pl.ds(sub, sub)], tok.at[1, mine], load_sem.at[5]),
        pltpu.make_async_copy(down_hbm, down_w, load_sem.at[6]),
    ]
    small = [
        pltpu.make_async_copy(src, dst, small_sem.at[i])
        for i, (src, dst) in enumerate(
            [
                (step_hbm, step),
                (write_hbm, write),
                (read_hbm, read),
                (seq_hbm, seq),
                (ids_hbm, ids),
                (route_hbm, route),
                (decay_hbm, decay_ref),
                (skip_hbm, skip_ref),
            ]
        )
    ]
    for load in loads[:6]:
        load.start()
    for load in small:
        load.start()

    barrier = pltpu.get_barrier_semaphore()
    for device in (partner, peer(1, half), peer(2, half), peer(3, half)):
        pl.semaphore_signal(barrier, inc=1, device_id=device, device_id_type=MESH)
    pl.semaphore_signal(barrier, inc=1, device_id=(inner, e), device_id_type=MESH)

    @pl.when(inside)
    def _():
        pl.semaphore_signal(barrier, inc=1, device_id=(outer, e), device_id_type=MESH)
        pl.semaphore_wait(barrier, 6)

    @pl.when(end)
    def _():
        pl.semaphore_wait(barrier, 5)

    def tok_rows(h):
        return tok_hbm.at[pl.ds(h * sub, sub)]

    to_partner = [
        remote(tok_rows(h), tok.at[h, mine], tsend.at[0], trecv.at[h], partner) for h in range(2)
    ]
    to_x = [
        remote(tok_rows(h), tok.at[2 + h, mine], tsend.at[0], trecv.at[2 + h], peer(1, half))
        for h in range(2)
    ]
    to_y = [
        remote(tok_rows(h), tok.at[4 + h, mine], tsend.at[0], trecv.at[4 + h], peer(2, half))
        for h in range(2)
    ]
    pass_x = [
        remote(
            tok.at[4 + h, mine_a], tok.at[6 + h, mine_a], tsend.at[0], trecv.at[6 + h],
            peer(1, half),
        )
        for h in range(2)
    ]
    pass_y = [
        remote(
            tok.at[2 + h, mine_b], tok.at[6 + h, mine_b], tsend.at[0], trecv.at[8 + h],
            peer(2, half),
        )
        for h in range(2)
    ]
    across = {
        n: remote(tok.at[n, mine], tok.at[n, mine], tsend.at[0], trecv.at[8 + n], partner)
        for n in range(2, UNITS)
    }
    for h in range(2):
        to_partner[h].start()
        to_x[h].start()
        to_y[h].start()

    def lend(k, begin=0, count=part):
        span = pl.ds(k * wide, wide)
        line = pl.ds(begin, count)
        return remote(
            down_hbm.at[opposite, line, span],
            far_w.at[line, span],
            wsend.at[0],
            wrecv.at[k],
            (inner, e),
        )

    @pl.when(end)
    def _():
        lend(0, 0, part // 2).start()

    whole = pl.ds(0, part)

    def own_in(n, span=whole):
        kind = jnp.where(end, 0, 1)
        return remote(
            hid.at[z, n, :, span],
            hid.at[z, n, :, span],
            own_in_send.at[0],
            hrecv.at[kind, n],
            (inner, e),
        )

    def own_out(n, span=whole):
        return remote(
            hid.at[z, n, :, span],
            hid.at[z, n, :, span],
            own_out_send.at[0],
            hrecv.at[0, n],
            (outer, e),
        )

    def fwd_in(n):
        return remote(
            hid.at[near, n], hid.at[near, n], fwd_in_send.at[0], hrecv.at[2, n], (inner, e)
        )

    def fwd_out(n):
        return remote(
            hid.at[far, n], hid.at[far, n], fwd_out_send.at[0], hrecv.at[1, n], (outer, e)
        )

    def fwd_end(n):
        return remote(
            hid.at[opposite, n],
            hid.at[opposite, n],
            fwd_end_send.at[0],
            hrecv.at[2, n],
            (outer, e),
        )

    def arrived(kind, j, n):
        remote(hid.at[j, n], hid.at[j, n], own_in_send.at[0], hrecv.at[kind, n], (near, e)).wait_recv()

    def state_copy():
        return remote(passed, came, ssend.at[0], srecv.at[0], (z + 1, e))

    def state_back():
        return remote(passed, came, ssend.at[0], srecv.at[0], (z - 1, e))

    head_count = step.shape[0]
    length = step.shape[1]
    state_count = write.shape[0]
    lanes = seq.shape[1]
    block_count = length // BLOCK
    lane_head = lax.broadcasted_iota(jnp.int32, (1, lanes), 1) // (lanes // head_count)

    mix_copy = pltpu.make_async_copy(mix_out, mix_hbm, load_sem.at[7])
    out_copy = pltpu.make_async_copy(out, out_hbm, load_sem.at[8])

    def mixer_first():
        for load in small:
            load.wait()
        down = lax.broadcasted_iota(jnp.int32, (BLOCK, BLOCK), 0)
        over = lax.broadcasted_iota(jnp.int32, (BLOCK, BLOCK), 1)
        lower = over <= down
        until = (down <= over).astype(F32)
        since = lower.astype(F32)
        head_row = lax.broadcasted_iota(jnp.int32, (head_count, 1), 0)
        rate = jnp.zeros((head_count, 1), F32)
        for h in range(head_count):
            rate = jnp.where(head_row == h, -jnp.exp(jnp.full((head_count, 1), decay_ref[h])), rate)
        state = jnp.zeros((state_count, lanes), F32)
        gone = jnp.zeros((1, lanes), F32)
        for k in range(block_count):
            span = pl.ds(k * BLOCK, BLOCK)
            steps = step[:, span]
            log_decay = steps * rate
            cumulative = jnp.dot(
                log_decay, until, precision=HIGHEST, preferred_element_type=F32
            )
            upright = lax.dot_general(
                since,
                log_decay,
                (((1,), (1,)), ((), ())),
                precision=HIGHEST,
                preferred_element_type=F32,
            )
            block_end = cumulative[:, BLOCK - 1 :]
            weights = jnp.exp(block_end - cumulative) * steps
            keys = write[:, span]
            scores = lax.dot_general(
                read[:, span], keys, (((0,), (0,)), ((), ())), preferred_element_type=F32
            )
            values = seq[span, :]
            mixed = jnp.zeros((BLOCK, lanes), F32)
            risen = jnp.zeros((BLOCK, lanes), F32)
            increment = jnp.zeros((state_count, lanes), F32)
            ends = jnp.zeros((1, lanes), F32)
            for h in range(head_count):
                here = lane_head == h
                difference = upright[:, h : h + 1] - cumulative[h : h + 1, :]
                decay = jnp.where(lower, jnp.exp(jnp.minimum(difference, 0.0)), 0.0)
                mixing = (scores * decay * steps[h : h + 1, :]).astype(BF16)
                mixed = jnp.where(
                    here, jnp.dot(mixing, values, preferred_element_type=F32), mixed
                )
                risen = jnp.where(here, upright[:, h : h + 1], risen)
                decayed = (keys.astype(F32) * weights[h : h + 1, :]).astype(BF16)
                increment = jnp.where(
                    here, jnp.dot(decayed, values, preferred_element_type=F32), increment
                )
                ends = jnp.where(here, block_end[h : h + 1, :], ends)
            local[span, :] = mixed
            grown[span, :] = jnp.exp(risen)
            entering[k] = state
            before[k] = jnp.broadcast_to(gone, (8, lanes))
            state = jnp.exp(ends) * state + increment
            gone = gone + ends
        final[...] = state
        before[block_count] = jnp.broadcast_to(gone, (8, lanes))

        @pl.when(z == 0)
        def _():
            came[...] = jnp.zeros((state_count, lanes), F32)
            passed[...] = state
            state_copy().start()

    def mixer_pass():
        state_back().wait_recv()
        passed[...] = jnp.exp(before[block_count][0:1, :]) * came[...] + final[...]
        state_copy().start()

    def mixer_second():
        @pl.when(z == LINES - 1)
        def _():
            state_back().wait_recv()

        state = came[...]
        gain = jnp.zeros((1, lanes), F32)
        for h in range(head_count):
            gain = jnp.where(lane_head == h, skip_ref[h], gain)
        for k in range(block_count):
            span = pl.ds(k * BLOCK, BLOCK)
            full = jnp.exp(before[k][0:1, :]) * state + entering[k]
            carried = lax.dot_general(
                read[:, span].astype(F32),
                full,
                (((0,), (0,)), ((), ())),
                precision=HIGHEST,
                preferred_element_type=F32,
            )
            total = local[span, :] + carried * grown[span, :] + gain * seq[span, :].astype(F32)
            mix_out[span, :] = total.astype(mix_out.dtype)
        mix_copy.start()

    def make_share():
        token = lax.broadcasted_iota(jnp.int32, (sub, rows), 1)
        place = lax.broadcasted_iota(jnp.int32, (sub, rows), 0)
        for c in range(CHUNKS):
            qx = lax.rem(px + c % GRID, GRID)
            qy = lax.rem(py + c // GRID, GRID)
            chosen = jnp.where(ids[...] == qy * GRID + qx, route[...], 0.0)
            weight = jnp.sum(chosen, axis=0, keepdims=True)
            for h in range(2):
                column = jnp.sum(
                    jnp.where(token == place + h * sub, weight, 0.0), axis=1, keepdims=True
                )
                share[2 * c + h] = jnp.broadcast_to(column, (sub, 128))

    def add_down(j, n):
        acc[n] += jnp.dot(hid[j, n], down_w[j], preferred_element_type=F32)

    def make_hidden(n, span):
        x = tok[n]
        g = jnp.dot(x, gate_w[:, span], preferred_element_type=F32)
        u = jnp.dot(x, up_w[:, span], preferred_element_type=F32)
        hid[z, n, :, span] = (jax.nn.silu(g) * u).astype(BF16)

    def tokens_ready(t):
        if t < 2:
            loads[0 if t == 0 else 5].wait()
            to_partner[t].wait_recv()
        if t == 2 or t == 4:
            h = (t - 2) // 2
            to_x[h].wait_recv()
            across[2 + h].start()
            to_y[h].wait_recv()
            across[4 + h].start()
            pass_x[h].start()
            pass_y[h].start()
            across[2 + h].wait_recv()
        if t == 3 or t == 5:
            across[4 + (t - 3) // 2].wait_recv()
        if t >= 6:
            across[t].wait_recv()

    def tokens_ahead(t):
        if t == 6 or t == 7:
            pass_x[t - 6].wait_recv()
            pass_y[t - 6].wait_recv()
            across[t].start()

    def take_far(n):
        arrived(1, far, n)

        @pl.when(inside)
        def _():
            fwd_out(n).start()

        add_down(far, n)

    def add_opposite(n):
        arrived(2, opposite, n)

        @pl.when(inside)
        def _():
            for k in range(HELPED, UNITS):

                @pl.when(n == k)
                def _():
                    fwd_end(k).start()

        add_down(opposite, n)

    def take_near(n):
        arrived(0, near, n)

        @pl.when(inside)
        def _():
            fwd_in(n).start()

        add_down(near, n)

    def own_down(t, carry):
        n = unit_of(t)
        acc[n] = jnp.dot(hid[z, n], down_w[z], preferred_element_type=F32)
        return carry

    def exchange(n):
        return remote(acc.at[n, theirs], swap.at[n], xsend.at[0], xrecv.at[n], partner)

    def bring_home(n):
        return remote(acc.at[n, mine], ret.at[n - 2], bsend.at[0], brecv.at[0], peer(n // 2, half))

    def finish(n):
        exchange(n).wait_recv()
        acc[n, mine] += swap[n]

    def early_finish():
        for n in (0, 2, 4):
            finish(n)
            if n > 1:
                bring_home(n).start()

    def forward_step(t, carry):
        @pl.when(t == 2)
        def _():
            loads[6].wait()

        @pl.when((t > 1) & (t <= UNITS))
        def _():
            lax.fori_loop(jnp.where(t == 2, 0, t - 1), t, own_down, 0)

        @pl.when(t == 2)
        def _():
            mixer_first()

        @pl.when(((z == 1) & (t == 4)) | ((z == 2) & (t == 6)))
        def _():
            mixer_pass()

        @pl.when(inside & (t == 2))
        def _():
            take_near(0)
            take_far(0)

        @pl.when(t < UNITS)
        def _():
            n = unit_of(t)
            for k in range(UNITS):

                @pl.when(t == k)
                def _():
                    tokens_ready(k)
                    if k == 2:

                        @pl.when(inside)
                        def _():
                            take_near(1)

            @pl.when(t == 0)
            def _():
                loads[1].wait()
                loads[2].wait()

            make_hidden(n, left)

            @pl.when(t == 0)
            def _():
                own_in(0, left).start()

                @pl.when(inside)
                def _():
                    own_out(0, left).start()

                loads[3].wait()
                loads[4].wait()
                loads[6].start()

            make_hidden(n, right)

            @pl.when(t == 0)
            def _():
                own_in(0, right).start()

                @pl.when(inside)
                def _():
                    own_out(0, right).start()

            @pl.when(inside & (t > 0))
            def _():
                own_out(n).start()

            @pl.when((end & (t > 0)) | (t == 2) | (t == 3))
            def _():
                own_in(n).start()

            for k in range(UNITS):

                @pl.when(t == k)
                def _():
                    tokens_ahead(k + 1)

        @pl.when(end & (t == 1))
        def _():
            lend(0, part // 2, part - part // 2).start()

        @pl.when(end & (t == UNITS - 1))
        def _():
            for k in range(1, GROUPS):
                lend(k).start()

        @pl.when(inside & (t == UNITS))
        def _():
            def one(i, inner_carry):
                add_opposite(unit_of(i))
                return inner_carry

            lax.fori_loop(0, 4, one, 0)
            for n in (0, 2, 4):
                exchange(n).start()

        @pl.when(inside & (t == UNITS + 1))
        def _():
            early_finish()

        @pl.when(inside & (t > 3))
        def _():
            take_near(unit_of(t - 2))

        @pl.when(inside & ((t == 4) | (t == 6)))
        def _():
            take_far(t - 2)

        return carry

    lax.fori_loop(0, UNITS + 2, forward_step, 0)

    @pl.when(inside)
    def _():
        for n in (6, 7, 3, 5, 1):
            own_in(n).start()

    def exchange2(k):
        return remote(acc2.at[k, :, theirs], swap2.at[k], x2send.at[0], x2recv.at[k], partner)

    def bring_home2(k, c):
        return remote(
            acc2.at[k, pl.ds(2 * c, 2), mine],
            ret2.at[k, c - 1],
            b2send.at[0],
            b2recv.at[k],
            peer(c, half),
        )

    def edge_copy(k):
        return remote(edge.at[k], edge.at[k], rsend.at[0], rrecv.at[0], (outer, e))

    def helper_dot(k):
        for i in range(GROUPS):

            @pl.when(k == i)
            def _():
                lend(i).wait_recv()

        span = pl.ds(pl.multiple_of(k * wide, wide), wide)
        x = hid[opposite, pl.ds(0, HELPED)].reshape(HELPED * rows, part)
        product = jnp.dot(x, far_w[:, span], preferred_element_type=F32)
        acc2[k] = product.reshape(HELPED, rows, wide)
        exchange2(k).start()

    def helper_home(k):
        exchange2(k).wait_recv()
        acc2[k, :, mine] += swap2[k]
        for c in range(1, CHUNKS - 1):
            bring_home2(k, c).start()

    def helper_edge(k):
        remote(
            ret2.at[k], ret2.at[k], b2send.at[0], b2recv.at[k], peer(1, half)
        ).wait_recv()
        for h in range(2):
            total = share[h, :, 0:1] * acc2[k, h, mine]
            for c in range(1, CHUNKS - 1):
                total += share[2 * c + h, :, 0:1] * ret2[k, c - 1, h]
            edge[k, pl.ds(h * sub, sub)] = total.astype(edge.dtype)
        edge_copy(k).start()

    make_share()

    @pl.when(inside)
    def _():
        def one(i, carry):
            add_opposite(unit_of(i))
            return carry

        lax.fori_loop(4, HELPED, one, 0)

    @pl.when(end)
    def _():
        def near_one(n, carry):
            take_near(n)
            return carry

        lax.fori_loop(0, UNITS, near_one, 0)

        def far_one(i, carry):
            take_far(2 * i)
            return carry

        lax.fori_loop(0, 3, far_one, 0)
        for n in (0, 2, 4):
            exchange(n).start()
        early_finish()

    @pl.when(inside)
    def _():
        add_opposite(HELPED)
        helper_dot(0)
        helper_dot(1)
        helper_home(0)

    order = (6, 7, 3, 5, 1)
    home = (2, 4, 6, 6)

    def finish_step(s, carry):
        @pl.when((s == 1) | (end & (s == 0)))
        def _():
            add_opposite(HELPED + s)

        n = jnp.where(s < 4, HELPED + s - 2, jnp.where(s < 6, 2 * s - 5, 1))

        @pl.when((s > 1) & (s < 7))
        def _():
            take_far(n)
            exchange(n).start()

        @pl.when(inside)
        def _():
            @pl.when(s < 6)
            def _():
                helper_dot(s + 2)

            @pl.when(s < 7)
            def _():
                helper_home(s + 1)

        for i, unit in enumerate(order):

            @pl.when(s == i + 2)
            def _():
                finish(unit)

            if unit > 1:

                @pl.when(s == jnp.where(inside, home[i], i + 2))
                def _():
                    bring_home(unit).start()

        @pl.when(s == 0)
        def _():
            mixer_second()

        @pl.when(inside & (s > 6))
        def _():
            helper_edge(s - 7)

        return carry

    lax.fori_loop(0, GROUPS + 7, finish_step, 0)

    returned = remote(ret, ret, bsend.at[0], brecv.at[0], peer(1, half))
    returned.wait_recv()
    for h in range(2):
        total = share[h, :, 0:1] * acc[h, mine]
        for c in range(1, CHUNKS):
            n = 2 * c + h
            total += share[n, :, 0:1] * ret[n - 2]
        swap[h] = total

    edges = remote(edge, edge, rsend.at[0], rrecv.at[0], (near, e))

    @pl.when(end)
    def _():
        edges.wait_recv()
        for k in range(GROUPS):
            span = pl.ds(k * wide, wide)
            for h in range(2):
                line = pl.ds(h * sub, sub)
                out[line, span] = (swap[h, :, span] + edge[k, line].astype(F32)).astype(out.dtype)

    @pl.when(inside)
    def _():
        for h in range(2):
            out[pl.ds(h * sub, sub)] = swap[h].astype(out.dtype)

    out_copy.start()
    @pl.when(z < LINES - 1)
    def _():
        state_copy().wait_send()

    def sent(ref, ssem, device):
        remote(ref, ref, ssem.at[0], hrecv.at[0, 0], device).wait_send()

    sent(tok.at[pl.ds(0, UNITS - 1)], tsend, partner)
    sent(hid.at[z], own_in_send, (inner, e))
    sent(swap, xsend, partner)
    returned.wait_send()

    @pl.when(inside)
    def _():
        sent(hid.at[z], own_out_send, (outer, e))
        sent(hid.at[near], fwd_in_send, (inner, e))
        sent(hid.at[far], fwd_out_send, (outer, e))
        sent(hid.at[opposite, pl.ds(HELPED, UNITS - HELPED)], fwd_end_send, (outer, e))
        sent(swap2, x2send, partner)
        sent(ret2, b2send, partner)
        edges.wait_send()

    @pl.when(end)
    def _():
        sent(far_w, wsend, (inner, e))

    mix_copy.wait()
    out_copy.wait()


def fused(
    seq_inputs,
    step_size,
    write_map,
    read_map,
    decay_log,
    skip_gain,
    moe_tokens,
    expert_ids,
    route_weights,
    gate_proj,
    up_proj,
    down_proj,
):
    rows, width = moe_tokens.shape
    part = gate_proj.shape[2]
    columns = down_proj.shape[2]
    length, lanes = seq_inputs.shape
    state_count = write_map.shape[0]
    block_count = length // BLOCK
    sub = rows // 2
    wide = columns // GROUPS
    dma = pltpu.SemaphoreType.DMA
    hbm = pl.BlockSpec(memory_space=pl.ANY)
    results = pl.pallas_call(
        fused_kernel,
        out_shape=(
            jax.ShapeDtypeStruct(seq_inputs.shape, BF16),
            jax.ShapeDtypeStruct((rows, columns), BF16),
        ),
        in_specs=[hbm] * 12,
        out_specs=(hbm, hbm),
        scratch_shapes=[
            pltpu.VMEM(seq_inputs.shape, BF16),
            pltpu.VMEM((rows, columns), BF16),
            pltpu.VMEM((width, part), BF16),
            pltpu.VMEM((width, part), BF16),
            pltpu.VMEM((LINES, part, columns), BF16),
            pltpu.VMEM((UNITS, rows, width), BF16),
            pltpu.VMEM((LINES, UNITS, rows, part), BF16),
            pltpu.VMEM((UNITS, rows, columns), F32),
            pltpu.VMEM((UNITS, sub, columns), F32),
            pltpu.VMEM((UNITS - 2, sub, columns), F32),
            pltpu.VMEM((part, columns), BF16),
            pltpu.VMEM((GROUPS, HELPED, rows, wide), F32),
            pltpu.VMEM((GROUPS, HELPED, sub, wide), F32),
            pltpu.VMEM((GROUPS, CHUNKS - 2, 2, sub, wide), F32),
            pltpu.VMEM((GROUPS, rows, wide), BF16),
            pltpu.VMEM((2, rows), jnp.int32),
            pltpu.VMEM((2, rows), F32),
            pltpu.VMEM((UNITS, sub, 128), F32),
            pltpu.SMEM(decay_log.shape, F32),
            pltpu.SMEM(skip_gain.shape, F32),
            pltpu.VMEM(seq_inputs.shape, BF16),
            pltpu.VMEM(step_size.shape, F32),
            pltpu.VMEM(write_map.shape, BF16),
            pltpu.VMEM(read_map.shape, BF16),
            pltpu.VMEM((length, lanes), F32),
            pltpu.VMEM((length, lanes), F32),
            pltpu.VMEM((block_count, state_count, lanes), F32),
            pltpu.VMEM((block_count + 1, 8, lanes), F32),
            pltpu.VMEM((state_count, lanes), F32),
            pltpu.VMEM((state_count, lanes), F32),
            pltpu.VMEM((state_count, lanes), F32),
            dma((9,)),
            dma((8,)),
            dma((1,)),
            dma((16,)),
            dma((1,)),
            dma((1,)),
            dma((1,)),
            dma((1,)),
            dma((1,)),
            dma((3, UNITS)),
            dma((1,)),
            dma((GROUPS,)),
            dma((1,)),
            dma((1,)),
            dma((1,)),
            dma((UNITS,)),
            dma((1,)),
            dma((1,)),
            dma((1,)),
            dma((GROUPS,)),
            dma((1,)),
            dma((GROUPS,)),
            dma((1,)),
            dma((1,)),
        ],
        compiler_params=pltpu.CompilerParams(
            collective_id=0, has_side_effects=True, vmem_limit_bytes=VMEM_BYTES
        ),
    )(
        moe_tokens,
        expert_ids.T,
        route_weights.T,
        seq_inputs,
        step_size,
        write_map,
        read_map,
        decay_log,
        skip_gain,
        gate_proj[0],
        up_proj[0],
        down_proj[0].reshape(LINES, part, columns),
    )
    return hand_over(*results)


def hand_over_kernel(*refs):
    count = (len(refs) - 2) // 3
    sources, targets, held = refs[:count], refs[count : 2 * count], refs[2 * count : 3 * count]
    in_sem, out_sem = refs[3 * count :]
    pieces = in_sem.shape[1]
    loads, stores = [], []
    for i in range(count):
        step = held[i].shape[0] // pieces
        for k in range(pieces):
            line = pl.ds(k * step, step)
            loads.append(
                pltpu.make_async_copy(sources[i].at[line], held[i].at[line], in_sem.at[i, k])
            )
            stores.append(
                pltpu.make_async_copy(held[i].at[line], targets[i].at[line], out_sem.at[i, k])
            )
    for load in loads:
        load.start()
    for load, store in zip(loads, stores):
        load.wait()
        store.start()
    for store in stores:
        store.wait()


def hand_over(*arrays):
    hbm = pl.BlockSpec(memory_space=pltpu.HBM)
    pieces = 2
    dma = pltpu.SemaphoreType.DMA((len(arrays), pieces))
    return pl.pallas_call(
        hand_over_kernel,
        out_shape=tuple(jax.ShapeDtypeStruct(a.shape, a.dtype) for a in arrays),
        in_specs=[hbm] * len(arrays),
        out_specs=(hbm,) * len(arrays),
        scratch_shapes=[pltpu.VMEM(a.shape, a.dtype) for a in arrays] + [dma, dma],
        compiler_params=pltpu.CompilerParams(vmem_limit_bytes=VMEM_BYTES),
    )(*arrays)


def fits(moe_tokens, gate_proj, down_proj):
    return (
        lax.axis_size("exp") == PAIR * GRID * GRID
        and lax.axis_size("ctx") == LINES
        and gate_proj.shape[2] % 128 == 0
        and down_proj.shape[2] % 1024 == 0
        and moe_tokens.shape[0] == 128
    )


def on_device(
    seq_inputs,
    step_size,
    write_map,
    read_map,
    decay_log,
    skip_gain,
    moe_tokens,
    expert_ids,
    route_weights,
    gate_proj,
    up_proj,
    down_proj,
):
    if fits(moe_tokens, gate_proj, down_proj):
        return fused(
            seq_inputs,
            step_size,
            write_map,
            read_map,
            decay_log,
            skip_gain,
            moe_tokens,
            expert_ids,
            route_weights,
            gate_proj,
            up_proj,
            down_proj,
        )
    local_mix, cumulative, block_ends, entering, final = mixer_prepare(
        seq_inputs, step_size, write_map, read_map, decay_log
    )
    total_log = jnp.sum(block_ends, axis=1)
    head_count, state_count, head_width = final.shape
    logs = jnp.broadcast_to(total_log[:, None, None], (head_count, 8, head_width))
    packed = jnp.concatenate([final, logs], axis=1)
    gathered = lax.all_gather(packed, "ctx")
    expert_output = expert_block(
        moe_tokens, expert_ids, route_weights, gate_proj, up_proj, down_proj
    )
    place = lax.axis_index("ctx")
    state_before = jnp.zeros_like(final)
    for lap in range(lax.axis_size("ctx")):
        latter = gathered[lap]
        decay = jnp.exp(latter[:, state_count, 0])
        added = decay[:, None, None] * state_before + latter[:, :state_count]
        state_before = jnp.where(lap < place, added, state_before)
    mixer_output = mixer_finish(
        local_mix, cumulative, block_ends, entering, state_before, read_map, seq_inputs, skip_gain
    )
    return (mixer_output, expert_output)


def solution(mesh):
    return jax.shard_map(
        on_device,
        mesh=mesh,
        in_specs=(
            P("ctx", "exp"),
            P("exp", "ctx"),
            P(None, "ctx"),
            P(None, "ctx"),
            P("exp"),
            P("exp"),
            P("exp", None),
            P("exp", None),
            P("exp", None),
            P("exp", None, "ctx"),
            P("exp", None, "ctx"),
            P("exp", None, "ctx"),
        ),
        out_specs=(P("ctx", "exp"), P("exp", "ctx")),
        check_vma=False,
    )
```

```python
import jax
import jax.numpy as jnp
from jax import lax
from jax.experimental import pallas as pl
from jax.experimental.pallas import tpu as pltpu
from jax.sharding import PartitionSpec as P

BLOCK = 256


HIGHEST = lax.Precision.HIGHEST


def block_chain(running, pieces):
    decay, increment = pieces
    return (decay[:, None, None] * running + increment, running)


def mixer_prepare(seq_inputs, step_size, write_map, read_map, decay_log):
    length = seq_inputs.shape[0]
    head_count = step_size.shape[0]
    state_count = write_map.shape[0]
    head_width = seq_inputs.shape[1] // head_count
    block_count = length // BLOCK
    decay_rate = -jnp.exp(decay_log)
    log_decay = (step_size * decay_rate[:, None]).reshape(head_count, block_count, BLOCK)
    order = lax.broadcasted_iota(jnp.int32, (BLOCK, BLOCK), 0)
    until = (order <= lax.broadcasted_iota(jnp.int32, (BLOCK, BLOCK), 1)).astype(jnp.float32)
    cumulative = jnp.einsum("hks,st->hkt", log_decay, until, precision=HIGHEST)
    block_ends = cumulative[:, :, BLOCK - 1]
    step_blocks = step_size.reshape(head_count, block_count, BLOCK)
    write_blocks = write_map.reshape(state_count, block_count, BLOCK)
    read_blocks = read_map.reshape(state_count, block_count, BLOCK)
    value_blocks = seq_inputs.reshape(block_count, BLOCK, head_count, head_width)
    scores = jnp.einsum(
        "nkt,nks->kts", read_blocks, write_blocks, preferred_element_type=jnp.float32
    )
    row_index = lax.broadcasted_iota(jnp.int32, (BLOCK, BLOCK), 0)
    column_index = lax.broadcasted_iota(jnp.int32, (BLOCK, BLOCK), 1)
    lower = column_index <= row_index
    difference = cumulative[:, :, :, None] - cumulative[:, :, None, :]
    decay = jnp.where(lower[None, None], jnp.exp(jnp.minimum(difference, 0.0)), 0.0)
    mixing = (scores[None] * decay * step_blocks[:, :, None, :]).astype(jnp.bfloat16)
    local_mix = jnp.einsum(
        "hkts,kshp->kthp", mixing, value_blocks, preferred_element_type=jnp.float32
    )
    weights = jnp.exp(block_ends[:, :, None] - cumulative) * step_blocks
    key_decayed = (write_blocks[None] * weights[:, None]).astype(jnp.bfloat16)
    increments = jnp.einsum(
        "hnks,kshp->khnp", key_decayed, value_blocks, preferred_element_type=jnp.float32
    )
    zero_state = jnp.zeros((head_count, state_count, head_width), jnp.float32)
    final, entering = lax.scan(block_chain, zero_state, (jnp.exp(block_ends).T, increments))
    return (local_mix, cumulative, block_ends, entering, final)


def mixer_finish(
    local_mix, cumulative, block_ends, entering, state_before, read_map, seq_inputs, skip_gain
):
    head_count = block_ends.shape[0]
    block_count = block_ends.shape[1]
    state_count = read_map.shape[0]
    head_width = entering.shape[3]
    before = jnp.cumsum(block_ends, axis=1) - block_ends
    states = jnp.exp(before).T[:, :, None, None] * state_before[None] + entering
    read_blocks = read_map.reshape(state_count, block_count, BLOCK).astype(jnp.float32)
    carried = jnp.einsum("nkt,khnp->kthp", read_blocks, states, precision=HIGHEST)
    carried = carried * jnp.exp(cumulative).transpose(1, 2, 0)[:, :, :, None]
    value_blocks = seq_inputs.reshape(block_count, BLOCK, head_count, head_width).astype(
        jnp.float32
    )
    output = local_mix + carried + skip_gain[None, None, :, None] * value_blocks
    return output.reshape(seq_inputs.shape).astype(jnp.bfloat16)


def expert_block(moe_tokens, expert_ids, route_weights, gate_proj, up_proj, down_proj):
    group_size = moe_tokens.shape[0]
    model_width = moe_tokens.shape[1]
    expert_count = lax.axis_size("exp") // 2
    capacity = min(group_size, 4 * group_size // expert_count)
    slot_count = expert_count * capacity
    assigned = expert_ids.reshape(group_size * 2)
    onehot = (
        assigned[:, None] == lax.broadcasted_iota(jnp.int32, (group_size * 2, expert_count), 1)
    ).astype(jnp.int32)
    earlier_count = jnp.cumsum(onehot, axis=0) - onehot
    position = jnp.sum((earlier_count + assigned[:, None] * capacity) * onehot, axis=1)
    matches = (
        position[:, None] == lax.broadcasted_iota(jnp.int32, (group_size * 2, slot_count), 1)
    ).astype(jnp.float32)
    dispatch = jnp.sum(matches.reshape(group_size, 2, slot_count), axis=1).astype(jnp.bfloat16)
    combine = jnp.sum(
        (matches * route_weights.reshape(group_size * 2)[:, None]).reshape(
            group_size, 2, slot_count
        ),
        axis=1,
    )
    gate_weight = gate_proj[0]
    up_weight = up_proj[0]
    down_weight = down_proj[0]
    packed = jnp.einsum(
        "is,id->sd", dispatch, moe_tokens, preferred_element_type=jnp.float32
    ).astype(jnp.bfloat16)
    doubled = jnp.broadcast_to(
        packed.reshape(expert_count, 1, capacity, model_width),
        (expert_count, 2, capacity, model_width),
    )
    arrived = lax.all_to_all(
        doubled.reshape(2 * slot_count, model_width), "exp", split_axis=0, concat_axis=0, tiled=True
    )
    gate_sums = jnp.dot(arrived, gate_weight, preferred_element_type=jnp.float32)
    up_sums = jnp.dot(arrived, up_weight, preferred_element_type=jnp.float32)
    hidden = (jax.nn.silu(gate_sums) * up_sums).astype(jnp.bfloat16)
    partial_out = jnp.dot(
        lax.all_gather(hidden, "ctx", axis=1, tiled=True),
        down_weight,
        preferred_element_type=jnp.float32,
    )
    returned = lax.all_to_all(partial_out, "exp", split_axis=0, concat_axis=0, tiled=True)
    summed = jnp.sum(returned.reshape(expert_count, 2, capacity, -1), axis=1).reshape(
        slot_count, -1
    )
    result = jnp.dot(combine, summed, precision=HIGHEST, preferred_element_type=jnp.float32)
    return result.astype(jnp.bfloat16)


MESH = pl.DeviceIdType.MESH
VMEM_BYTES = 58 * 2**20
GRID = 2
PAIR = 2
LINES = 4
CHUNKS = GRID * GRID
UNITS = 2 * CHUNKS
GROUPS = 8
HELPED = UNITS - 2
F32 = jnp.float32
BF16 = jnp.bfloat16


def unit_of(t):
    return jnp.where(t == 3, 4, jnp.where(t == 4, 3, t))


def fused_kernel(
    tok_hbm,
    ids_hbm,
    route_hbm,
    seq_hbm,
    step_hbm,
    write_hbm,
    read_hbm,
    decay_hbm,
    skip_hbm,
    gate_hbm,
    up_hbm,
    down_hbm,
    mix_hbm,
    out_hbm,
    mix_out,
    out,
    gate_w,
    up_w,
    down_w,
    tok,
    hid,
    acc,
    swap,
    ret,
    far_w,
    acc2,
    swap2,
    ret2,
    edge,
    ids,
    route,
    share,
    decay_ref,
    skip_ref,
    seq,
    step,
    write,
    read,
    local,
    grown,
    entering,
    before,
    final,
    came,
    passed,
    load_sem,
    small_sem,
    tsend,
    trecv,
    own_in_send,
    own_out_send,
    fwd_in_send,
    fwd_out_send,
    fwd_end_send,
    hrecv,
    wsend,
    wrecv,
    rsend,
    rrecv,
    xsend,
    xrecv,
    bsend,
    brecv,
    x2send,
    x2recv,
    b2send,
    b2recv,
    ssend,
    srecv,
):
    z = lax.axis_index("ctx")
    e = lax.axis_index("exp")
    half = lax.rem(e, PAIR)
    other = 1 - half
    px = lax.rem(e // PAIR, GRID)
    py = e // (PAIR * GRID)
    rows = tok.shape[1]
    sub = rows // 2
    quarter = sub // 2
    part = gate_w.shape[1]
    first = part // 256 * 128
    columns = acc.shape[2]
    wide = columns // GROUPS

    end = (z == 0) | (z == LINES - 1)
    inside = (z > 0) & (z < LINES - 1)
    low = z < 2
    inner = jnp.where(low, z + 1, z - 1)
    outer = jnp.where(low, z - 1, z + 1)
    near = jnp.where(end, inner, outer)
    far = jnp.where(end, LINES - 1 - inner, inner)
    opposite = jnp.where(low, LINES - 1, 0)

    def peer(c, core):
        qx = lax.rem(px + c % GRID, GRID)
        qy = lax.rem(py + c // GRID, GRID)
        return (z, (qy * GRID + qx) * PAIR + core)

    partner = peer(0, other)
    mine = pl.ds(pl.multiple_of(half * sub, sub), sub)
    theirs = pl.ds(pl.multiple_of(other * sub, sub), sub)
    mine_a = pl.ds(pl.multiple_of(half * sub, quarter), quarter)
    mine_b = pl.ds(pl.multiple_of(half * sub + quarter, quarter), quarter)

    def remote(src, dst, ssem, rsem, device):
        return pltpu.make_async_remote_copy(
            src_ref=src,
            dst_ref=dst,
            send_sem=ssem,
            recv_sem=rsem,
            device_id=device,
            device_id_type=MESH,
        )

    left, right = pl.ds(0, first), pl.ds(first, part - first)
    loads = [
        pltpu.make_async_copy(tok_hbm.at[pl.ds(0, sub)], tok.at[0, mine], load_sem.at[0]),
        pltpu.make_async_copy(gate_hbm.at[:, left], gate_w.at[:, left], load_sem.at[1]),
        pltpu.make_async_copy(up_hbm.at[:, left], up_w.at[:, left], load_sem.at[2]),
        pltpu.make_async_copy(gate_hbm.at[:, right], gate_w.at[:, right], load_sem.at[3]),
        pltpu.make_async_copy(up_hbm.at[:, right], up_w.at[:, right], load_sem.at[4]),
        pltpu.make_async_copy(tok_hbm.at[pl.ds(sub, sub)], tok.at[1, mine], load_sem.at[5]),
        pltpu.make_async_copy(down_hbm, down_w, load_sem.at[6]),
    ]
    small = [
        pltpu.make_async_copy(src, dst, small_sem.at[i])
        for i, (src, dst) in enumerate(
            [
                (step_hbm, step),
                (write_hbm, write),
                (read_hbm, read),
                (seq_hbm, seq),
                (ids_hbm, ids),
                (route_hbm, route),
                (decay_hbm, decay_ref),
                (skip_hbm, skip_ref),
            ]
        )
    ]
    barrier = pltpu.get_barrier_semaphore()
    for device in (partner, peer(1, half), peer(2, half), peer(3, half)):
        pl.semaphore_signal(barrier, inc=1, device_id=device, device_id_type=MESH)
    pl.semaphore_signal(barrier, inc=1, device_id=(inner, e), device_id_type=MESH)

    @pl.when(inside)
    def _():
        pl.semaphore_signal(barrier, inc=1, device_id=(outer, e), device_id_type=MESH)

    for load in loads[:6]:
        load.start()
    for load in small:
        load.start()

    @pl.when(inside)
    def _():
        pl.semaphore_wait(barrier, 6)

    @pl.when(end)
    def _():
        pl.semaphore_wait(barrier, 5)

    def tok_rows(h):
        return tok_hbm.at[pl.ds(h * sub, sub)]

    to_partner = [
        remote(tok_rows(h), tok.at[h, mine], tsend.at[0], trecv.at[h], partner) for h in range(2)
    ]
    to_x = [
        remote(tok_rows(h), tok.at[2 + h, mine], tsend.at[0], trecv.at[2 + h], peer(1, half))
        for h in range(2)
    ]
    to_y = [
        remote(tok_rows(h), tok.at[4 + h, mine], tsend.at[0], trecv.at[4 + h], peer(2, half))
        for h in range(2)
    ]
    pass_x = [
        remote(
            tok.at[4 + h, mine_a], tok.at[6 + h, mine_a], tsend.at[0], trecv.at[6 + h],
            peer(1, half),
        )
        for h in range(2)
    ]
    pass_y = [
        remote(
            tok.at[2 + h, mine_b], tok.at[6 + h, mine_b], tsend.at[0], trecv.at[8 + h],
            peer(2, half),
        )
        for h in range(2)
    ]
    across = {
        n: remote(tok.at[n, mine], tok.at[n, mine], tsend.at[0], trecv.at[8 + n], partner)
        for n in range(2, UNITS)
    }
    for h in range(2):
        to_partner[h].start()
        to_x[h].start()
        to_y[h].start()

    def lend(k, begin=0, count=part):
        span = pl.ds(k * wide, wide)
        line = pl.ds(begin, count)
        return remote(
            down_hbm.at[opposite, line, span],
            far_w.at[line, span],
            wsend.at[0],
            wrecv.at[k],
            (inner, e),
        )

    @pl.when(end)
    def _():
        lend(0, 0, part // 2).start()

    whole = pl.ds(0, part)

    def own_in(n, span=whole):
        kind = jnp.where(end, 0, 1)
        return remote(
            hid.at[z, n, :, span],
            hid.at[z, n, :, span],
            own_in_send.at[0],
            hrecv.at[kind, n],
            (inner, e),
        )

    def own_out(n, span=whole):
        return remote(
            hid.at[z, n, :, span],
            hid.at[z, n, :, span],
            own_out_send.at[0],
            hrecv.at[0, n],
            (outer, e),
        )

    def fwd_in(n):
        return remote(
            hid.at[near, n], hid.at[near, n], fwd_in_send.at[0], hrecv.at[2, n], (inner, e)
        )

    def fwd_out(n):
        return remote(
            hid.at[far, n], hid.at[far, n], fwd_out_send.at[0], hrecv.at[1, n], (outer, e)
        )

    def fwd_end(n):
        return remote(
            hid.at[opposite, n],
            hid.at[opposite, n],
            fwd_end_send.at[0],
            hrecv.at[2, n],
            (outer, e),
        )

    def arrived(kind, j, n):
        remote(hid.at[j, n], hid.at[j, n], own_in_send.at[0], hrecv.at[kind, n], (near, e)).wait_recv()

    def state_copy():
        return remote(passed, came, ssend.at[0], srecv.at[0], (z + 1, e))

    def state_back():
        return remote(passed, came, ssend.at[0], srecv.at[0], (z - 1, e))

    head_count = step.shape[0]
    length = step.shape[1]
    state_count = write.shape[0]
    lanes = seq.shape[1]
    block_count = length // BLOCK
    lane_head = lax.broadcasted_iota(jnp.int32, (1, lanes), 1) // (lanes // head_count)

    mix_copy = pltpu.make_async_copy(mix_out, mix_hbm, load_sem.at[7])
    out_copy = pltpu.make_async_copy(out, out_hbm, load_sem.at[8])

    def mixer_first():
        for load in small:
            load.wait()
        down = lax.broadcasted_iota(jnp.int32, (BLOCK, BLOCK), 0)
        over = lax.broadcasted_iota(jnp.int32, (BLOCK, BLOCK), 1)
        lower = over <= down
        until = (down <= over).astype(F32)
        since = lower.astype(F32)
        head_row = lax.broadcasted_iota(jnp.int32, (head_count, 1), 0)
        rate = jnp.zeros((head_count, 1), F32)
        for h in range(head_count):
            rate = jnp.where(head_row == h, -jnp.exp(jnp.full((head_count, 1), decay_ref[h])), rate)
        state = jnp.zeros((state_count, lanes), F32)
        gone = jnp.zeros((1, lanes), F32)
        for k in range(block_count):
            span = pl.ds(k * BLOCK, BLOCK)
            steps = step[:, span]
            log_decay = steps * rate
            cumulative = jnp.dot(
                log_decay, until, precision=HIGHEST, preferred_element_type=F32
            )
            upright = lax.dot_general(
                since,
                log_decay,
                (((1,), (1,)), ((), ())),
                precision=HIGHEST,
                preferred_element_type=F32,
            )
            block_end = cumulative[:, BLOCK - 1 :]
            weights = jnp.exp(block_end - cumulative) * steps
            keys = write[:, span]
            scores = lax.dot_general(
                read[:, span], keys, (((0,), (0,)), ((), ())), preferred_element_type=F32
            )
            values = seq[span, :]
            mixed = jnp.zeros((BLOCK, lanes), F32)
            risen = jnp.zeros((BLOCK, lanes), F32)
            increment = jnp.zeros((state_count, lanes), F32)
            ends = jnp.zeros((1, lanes), F32)
            for h in range(head_count):
                here = lane_head == h
                difference = upright[:, h : h + 1] - cumulative[h : h + 1, :]
                decay = jnp.where(lower, jnp.exp(jnp.minimum(difference, 0.0)), 0.0)
                mixing = (scores * decay * steps[h : h + 1, :]).astype(BF16)
                mixed = jnp.where(
                    here, jnp.dot(mixing, values, preferred_element_type=F32), mixed
                )
                risen = jnp.where(here, upright[:, h : h + 1], risen)
                decayed = (keys.astype(F32) * weights[h : h + 1, :]).astype(BF16)
                increment = jnp.where(
                    here, jnp.dot(decayed, values, preferred_element_type=F32), increment
                )
                ends = jnp.where(here, block_end[h : h + 1, :], ends)
            local[span, :] = mixed
            grown[span, :] = jnp.exp(risen)
            entering[k] = state
            before[k] = jnp.broadcast_to(gone, (8, lanes))
            state = jnp.exp(ends) * state + increment
            gone = gone + ends
        final[...] = state
        before[block_count] = jnp.broadcast_to(gone, (8, lanes))

        @pl.when(z == 0)
        def _():
            came[...] = jnp.zeros((state_count, lanes), F32)
            passed[...] = state
            state_copy().start()

    def mixer_pass():
        state_back().wait_recv()
        passed[...] = jnp.exp(before[block_count][0:1, :]) * came[...] + final[...]
        state_copy().start()

    def mixer_second():
        @pl.when(z == LINES - 1)
        def _():
            state_back().wait_recv()

        state = came[...]
        gain = jnp.zeros((1, lanes), F32)
        for h in range(head_count):
            gain = jnp.where(lane_head == h, skip_ref[h], gain)
        for k in range(block_count):
            span = pl.ds(k * BLOCK, BLOCK)
            full = jnp.exp(before[k][0:1, :]) * state + entering[k]
            carried = lax.dot_general(
                read[:, span].astype(F32),
                full,
                (((0,), (0,)), ((), ())),
                precision=HIGHEST,
                preferred_element_type=F32,
            )
            total = local[span, :] + carried * grown[span, :] + gain * seq[span, :].astype(F32)
            mix_out[span, :] = total.astype(mix_out.dtype)
        mix_copy.start()

    def make_share():
        token = lax.broadcasted_iota(jnp.int32, (sub, rows), 1)
        place = lax.broadcasted_iota(jnp.int32, (sub, rows), 0)
        for c in range(CHUNKS):
            qx = lax.rem(px + c % GRID, GRID)
            qy = lax.rem(py + c // GRID, GRID)
            chosen = jnp.where(ids[...] == qy * GRID + qx, route[...], 0.0)
            weight = jnp.sum(chosen, axis=0, keepdims=True)
            for h in range(2):
                column = jnp.sum(
                    jnp.where(token == place + h * sub, weight, 0.0), axis=1, keepdims=True
                )
                share[2 * c + h] = jnp.broadcast_to(column, (sub, 128))

    def add_down(j, n):
        acc[n] += jnp.dot(hid[j, n], down_w[j], preferred_element_type=F32)

    def make_hidden(n, span):
        x = tok[n]
        g = jnp.dot(x, gate_w[:, span], preferred_element_type=F32)
        u = jnp.dot(x, up_w[:, span], preferred_element_type=F32)
        hid[z, n, :, span] = (jax.nn.silu(g) * u).astype(BF16)

    def tokens_ready(t):
        if t < 2:
            loads[0 if t == 0 else 5].wait()
            to_partner[t].wait_recv()
        if t == 2 or t == 4:
            h = (t - 2) // 2
            to_x[h].wait_recv()
            across[2 + h].start()
            to_y[h].wait_recv()
            across[4 + h].start()
            pass_x[h].start()
            pass_y[h].start()
            across[2 + h].wait_recv()
        if t == 3 or t == 5:
            across[4 + (t - 3) // 2].wait_recv()
        if t >= 6:
            across[t].wait_recv()

    def tokens_ahead(t):
        if t == 6 or t == 7:
            pass_x[t - 6].wait_recv()
            pass_y[t - 6].wait_recv()
            across[t].start()

    def take_far(n):
        arrived(1, far, n)

        @pl.when(inside)
        def _():
            fwd_out(n).start()

        add_down(far, n)

    def add_opposite(n):
        arrived(2, opposite, n)

        @pl.when(inside)
        def _():
            for k in range(HELPED, UNITS):

                @pl.when(n == k)
                def _():
                    fwd_end(k).start()

        add_down(opposite, n)

    def take_near(n):
        arrived(0, near, n)

        @pl.when(inside)
        def _():
            fwd_in(n).start()

        add_down(near, n)

    def own_down(t, carry):
        n = unit_of(t)
        acc[n] = jnp.dot(hid[z, n], down_w[z], preferred_element_type=F32)
        return carry

    def exchange(n):
        return remote(acc.at[n, theirs], swap.at[n], xsend.at[0], xrecv.at[n], partner)

    def bring_home(n):
        return remote(acc.at[n, mine], ret.at[n - 2], bsend.at[0], brecv.at[0], peer(n // 2, half))

    def finish(n):
        exchange(n).wait_recv()
        acc[n, mine] += swap[n]

    def early_finish():
        for n in (0, 2, 4):
            finish(n)
            if n > 1:
                bring_home(n).start()

    def forward_step(t, carry):
        @pl.when(t == 2)
        def _():
            loads[6].wait()

        @pl.when((t > 1) & (t <= UNITS))
        def _():
            lax.fori_loop(jnp.where(t == 2, 0, t - 1), t, own_down, 0)

        @pl.when(t == 2)
        def _():
            mixer_first()

        @pl.when(((z == 1) & (t == 4)) | ((z == 2) & (t == 6)))
        def _():
            mixer_pass()

        @pl.when(inside & (t == 2))
        def _():
            take_near(0)
            take_far(0)

        @pl.when(t < UNITS)
        def _():
            n = unit_of(t)
            for k in range(UNITS):

                @pl.when(t == k)
                def _():
                    tokens_ready(k)
                    if k == 2:

                        @pl.when(inside)
                        def _():
                            arrived(0, near, 1)
                            fwd_in(1).start()

            @pl.when(t == 0)
            def _():
                loads[1].wait()
                loads[2].wait()

            make_hidden(n, left)

            @pl.when(t == 0)
            def _():
                own_in(0, left).start()

                @pl.when(inside)
                def _():
                    own_out(0, left).start()

                loads[3].wait()
                loads[4].wait()
                loads[6].start()

            make_hidden(n, right)

            @pl.when(t == 0)
            def _():
                own_in(0, right).start()

                @pl.when(inside)
                def _():
                    own_out(0, right).start()

            @pl.when(inside & (t > 0))
            def _():
                own_out(n).start()

            @pl.when((end & (t > 0)) | (t == 2) | (t == 3))
            def _():
                own_in(n).start()

            for k in range(UNITS):

                @pl.when(t == k)
                def _():
                    tokens_ahead(k + 1)

        @pl.when(end & (t == 1))
        def _():
            lend(0, part // 2, part - part // 2).start()

        @pl.when(end & (t == UNITS - 1))
        def _():
            for k in range(1, GROUPS):
                lend(k).start()

        @pl.when(inside & (t == UNITS))
        def _():
            def one(i, inner_carry):
                add_opposite(unit_of(i))
                return inner_carry

            lax.fori_loop(0, 4, one, 0)
            for n in (0, 2, 4):
                exchange(n).start()

        @pl.when(inside & (t == UNITS + 1))
        def _():
            early_finish()

        @pl.when(inside & (t > 3))
        def _():
            take_near(unit_of(t - 2))

        @pl.when(inside & (t == 2))
        def _():
            add_down(near, 1)

        @pl.when(inside & ((t == 4) | (t == 6)))
        def _():
            take_far(t - 2)

        return carry

    lax.fori_loop(0, UNITS + 2, forward_step, 0)

    @pl.when(inside)
    def _():
        for n in (6, 7, 3, 5, 1):
            own_in(n).start()

    def exchange2(k):
        return remote(acc2.at[k, :, theirs], swap2.at[k], x2send.at[0], x2recv.at[k], partner)

    def bring_home2(k, c):
        return remote(
            acc2.at[k, pl.ds(2 * c, 2), mine],
            ret2.at[k, c - 1],
            b2send.at[0],
            b2recv.at[k],
            peer(c, half),
        )

    def edge_copy(k):
        return remote(edge.at[k], edge.at[k], rsend.at[0], rrecv.at[0], (outer, e))

    def helper_dot(k):
        for i in range(GROUPS):

            @pl.when(k == i)
            def _():
                lend(i).wait_recv()

        span = pl.ds(pl.multiple_of(k * wide, wide), wide)
        x = hid[opposite, pl.ds(0, HELPED)].reshape(HELPED * rows, part)
        product = jnp.dot(x, far_w[:, span], preferred_element_type=F32)
        acc2[k] = product.reshape(HELPED, rows, wide)
        exchange2(k).start()

    def helper_home(k):
        exchange2(k).wait_recv()
        acc2[k, :, mine] += swap2[k]
        for c in range(1, CHUNKS - 1):
            bring_home2(k, c).start()

    def helper_edge(k):
        remote(
            ret2.at[k], ret2.at[k], b2send.at[0], b2recv.at[k], peer(1, half)
        ).wait_recv()
        for h in range(2):
            total = share[h, :, 0:1] * acc2[k, h, mine]
            for c in range(1, CHUNKS - 1):
                total += share[2 * c + h, :, 0:1] * ret2[k, c - 1, h]
            edge[k, pl.ds(h * sub, sub)] = total.astype(edge.dtype)
        edge_copy(k).start()

    make_share()

    @pl.when(inside)
    def _():
        def one(i, carry):
            add_opposite(unit_of(i))
            return carry

        lax.fori_loop(4, HELPED, one, 0)

    @pl.when(end)
    def _():
        def near_one(n, carry):
            take_near(n)
            return carry

        lax.fori_loop(0, UNITS, near_one, 0)

        def far_one(i, carry):
            take_far(2 * i)
            return carry

        lax.fori_loop(0, 3, far_one, 0)
        for n in (0, 2, 4):
            exchange(n).start()
        early_finish()

    @pl.when(inside)
    def _():
        add_opposite(HELPED)
        helper_dot(0)
        helper_dot(1)
        helper_home(0)

    order = (6, 7, 3, 5, 1)
    home = (2, 4, 6, 6)

    def finish_step(s, carry):
        @pl.when((s == 1) | (end & (s == 0)))
        def _():
            add_opposite(HELPED + s)

        n = jnp.where(s < 4, HELPED + s - 2, jnp.where(s < 6, 2 * s - 5, 1))

        @pl.when((s > 1) & (s < 7))
        def _():
            take_far(n)
            exchange(n).start()

        @pl.when(inside)
        def _():
            @pl.when(s < 6)
            def _():
                helper_dot(s + 2)

            @pl.when(s < 7)
            def _():
                helper_home(s + 1)

        for i, unit in enumerate(order):

            @pl.when(s == i + 2)
            def _():
                finish(unit)

            if unit > 1:

                @pl.when(s == jnp.where(inside, home[i], i + 2))
                def _():
                    bring_home(unit).start()

        @pl.when(s == 0)
        def _():
            mixer_second()

        @pl.when(inside & (s > 6))
        def _():
            helper_edge(s - 7)

        return carry

    lax.fori_loop(0, GROUPS + 7, finish_step, 0)

    returned = remote(ret, ret, bsend.at[0], brecv.at[0], peer(1, half))
    returned.wait_recv()
    for h in range(2):
        total = share[h, :, 0:1] * acc[h, mine]
        for c in range(1, CHUNKS):
            n = 2 * c + h
            total += share[n, :, 0:1] * ret[n - 2]
        swap[h] = total

    edges = remote(edge, edge, rsend.at[0], rrecv.at[0], (near, e))

    @pl.when(end)
    def _():
        edges.wait_recv()
        for k in range(GROUPS):
            span = pl.ds(k * wide, wide)
            for h in range(2):
                line = pl.ds(h * sub, sub)
                out[line, span] = (swap[h, :, span] + edge[k, line].astype(F32)).astype(out.dtype)

    @pl.when(inside)
    def _():
        for h in range(2):
            out[pl.ds(h * sub, sub)] = swap[h].astype(out.dtype)

    out_copy.start()
    @pl.when(z < LINES - 1)
    def _():
        state_copy().wait_send()

    def sent(ref, ssem, device):
        remote(ref, ref, ssem.at[0], hrecv.at[0, 0], device).wait_send()

    sent(tok.at[pl.ds(0, UNITS - 1)], tsend, partner)
    sent(hid.at[z], own_in_send, (inner, e))
    sent(swap, xsend, partner)
    returned.wait_send()

    @pl.when(inside)
    def _():
        sent(hid.at[z], own_out_send, (outer, e))
        sent(hid.at[near], fwd_in_send, (inner, e))
        sent(hid.at[far], fwd_out_send, (outer, e))
        sent(hid.at[opposite, pl.ds(HELPED, UNITS - HELPED)], fwd_end_send, (outer, e))
        sent(swap2, x2send, partner)
        sent(ret2, b2send, partner)
        edges.wait_send()

    @pl.when(end)
    def _():
        sent(far_w, wsend, (inner, e))

    mix_copy.wait()
    out_copy.wait()


def fused(
    seq_inputs,
    step_size,
    write_map,
    read_map,
    decay_log,
    skip_gain,
    moe_tokens,
    expert_ids,
    route_weights,
    gate_proj,
    up_proj,
    down_proj,
):
    rows, width = moe_tokens.shape
    part = gate_proj.shape[2]
    columns = down_proj.shape[2]
    length, lanes = seq_inputs.shape
    state_count = write_map.shape[0]
    block_count = length // BLOCK
    sub = rows // 2
    wide = columns // GROUPS
    dma = pltpu.SemaphoreType.DMA
    hbm = pl.BlockSpec(memory_space=pl.ANY)
    results = pl.pallas_call(
        fused_kernel,
        out_shape=(
            jax.ShapeDtypeStruct(seq_inputs.shape, BF16),
            jax.ShapeDtypeStruct((rows, columns), BF16),
        ),
        in_specs=[hbm] * 12,
        out_specs=(hbm, hbm),
        scratch_shapes=[
            pltpu.VMEM(seq_inputs.shape, BF16),
            pltpu.VMEM((rows, columns), BF16),
            pltpu.VMEM((width, part), BF16),
            pltpu.VMEM((width, part), BF16),
            pltpu.VMEM((LINES, part, columns), BF16),
            pltpu.VMEM((UNITS, rows, width), BF16),
            pltpu.VMEM((LINES, UNITS, rows, part), BF16),
            pltpu.VMEM((UNITS, rows, columns), F32),
            pltpu.VMEM((UNITS, sub, columns), F32),
            pltpu.VMEM((UNITS - 2, sub, columns), F32),
            pltpu.VMEM((part, columns), BF16),
            pltpu.VMEM((GROUPS, HELPED, rows, wide), F32),
            pltpu.VMEM((GROUPS, HELPED, sub, wide), F32),
            pltpu.VMEM((GROUPS, CHUNKS - 2, 2, sub, wide), F32),
            pltpu.VMEM((GROUPS, rows, wide), BF16),
            pltpu.VMEM((2, rows), jnp.int32),
            pltpu.VMEM((2, rows), F32),
            pltpu.VMEM((UNITS, sub, 128), F32),
            pltpu.SMEM(decay_log.shape, F32),
            pltpu.SMEM(skip_gain.shape, F32),
            pltpu.VMEM(seq_inputs.shape, BF16),
            pltpu.VMEM(step_size.shape, F32),
            pltpu.VMEM(write_map.shape, BF16),
            pltpu.VMEM(read_map.shape, BF16),
            pltpu.VMEM((length, lanes), F32),
            pltpu.VMEM((length, lanes), F32),
            pltpu.VMEM((block_count, state_count, lanes), F32),
            pltpu.VMEM((block_count + 1, 8, lanes), F32),
            pltpu.VMEM((state_count, lanes), F32),
            pltpu.VMEM((state_count, lanes), F32),
            pltpu.VMEM((state_count, lanes), F32),
            dma((9,)),
            dma((8,)),
            dma((1,)),
            dma((16,)),
            dma((1,)),
            dma((1,)),
            dma((1,)),
            dma((1,)),
            dma((1,)),
            dma((3, UNITS)),
            dma((1,)),
            dma((GROUPS,)),
            dma((1,)),
            dma((1,)),
            dma((1,)),
            dma((UNITS,)),
            dma((1,)),
            dma((1,)),
            dma((1,)),
            dma((GROUPS,)),
            dma((1,)),
            dma((GROUPS,)),
            dma((1,)),
            dma((1,)),
        ],
        compiler_params=pltpu.CompilerParams(
            collective_id=0, has_side_effects=True, vmem_limit_bytes=VMEM_BYTES
        ),
    )(
        moe_tokens,
        expert_ids.T,
        route_weights.T,
        seq_inputs,
        step_size,
        write_map,
        read_map,
        decay_log,
        skip_gain,
        gate_proj[0],
        up_proj[0],
        down_proj[0].reshape(LINES, part, columns),
    )
    return hand_over(*results)


def hand_over_kernel(*refs):
    count = (len(refs) - 2) // 3
    sources, targets, held = refs[:count], refs[count : 2 * count], refs[2 * count : 3 * count]
    in_sem, out_sem = refs[3 * count :]
    pieces = in_sem.shape[1]
    loads, stores = [], []
    for i in range(count):
        step = held[i].shape[0] // pieces
        for k in range(pieces):
            line = pl.ds(k * step, step)
            loads.append(
                pltpu.make_async_copy(sources[i].at[line], held[i].at[line], in_sem.at[i, k])
            )
            stores.append(
                pltpu.make_async_copy(held[i].at[line], targets[i].at[line], out_sem.at[i, k])
            )
    for load in loads:
        load.start()
    for load, store in zip(loads, stores):
        load.wait()
        store.start()
    for store in stores:
        store.wait()


def hand_over(*arrays):
    hbm = pl.BlockSpec(memory_space=pltpu.HBM)
    pieces = 2
    dma = pltpu.SemaphoreType.DMA((len(arrays), pieces))
    return pl.pallas_call(
        hand_over_kernel,
        out_shape=tuple(jax.ShapeDtypeStruct(a.shape, a.dtype) for a in arrays),
        in_specs=[hbm] * len(arrays),
        out_specs=(hbm,) * len(arrays),
        scratch_shapes=[pltpu.VMEM(a.shape, a.dtype) for a in arrays] + [dma, dma],
        compiler_params=pltpu.CompilerParams(vmem_limit_bytes=VMEM_BYTES),
    )(*arrays)


def fits(moe_tokens, gate_proj, down_proj):
    return (
        lax.axis_size("exp") == PAIR * GRID * GRID
        and lax.axis_size("ctx") == LINES
        and gate_proj.shape[2] % 128 == 0
        and down_proj.shape[2] % 1024 == 0
        and moe_tokens.shape[0] == 128
    )


def on_device(
    seq_inputs,
    step_size,
    write_map,
    read_map,
    decay_log,
    skip_gain,
    moe_tokens,
    expert_ids,
    route_weights,
    gate_proj,
    up_proj,
    down_proj,
):
    if fits(moe_tokens, gate_proj, down_proj):
        return fused(
            seq_inputs,
            step_size,
            write_map,
            read_map,
            decay_log,
            skip_gain,
            moe_tokens,
            expert_ids,
            route_weights,
            gate_proj,
            up_proj,
            down_proj,
        )
    local_mix, cumulative, block_ends, entering, final = mixer_prepare(
        seq_inputs, step_size, write_map, read_map, decay_log
    )
    total_log = jnp.sum(block_ends, axis=1)
    head_count, state_count, head_width = final.shape
    logs = jnp.broadcast_to(total_log[:, None, None], (head_count, 8, head_width))
    packed = jnp.concatenate([final, logs], axis=1)
    gathered = lax.all_gather(packed, "ctx")
    expert_output = expert_block(
        moe_tokens, expert_ids, route_weights, gate_proj, up_proj, down_proj
    )
    place = lax.axis_index("ctx")
    state_before = jnp.zeros_like(final)
    for lap in range(lax.axis_size("ctx")):
        latter = gathered[lap]
        decay = jnp.exp(latter[:, state_count, 0])
        added = decay[:, None, None] * state_before + latter[:, :state_count]
        state_before = jnp.where(lap < place, added, state_before)
    mixer_output = mixer_finish(
        local_mix, cumulative, block_ends, entering, state_before, read_map, seq_inputs, skip_gain
    )
    return (mixer_output, expert_output)


def solution(mesh):
    return jax.shard_map(
        on_device,
        mesh=mesh,
        in_specs=(
            P("ctx", "exp"),
            P("exp", "ctx"),
            P(None, "ctx"),
            P(None, "ctx"),
            P("exp"),
            P("exp"),
            P("exp", None),
            P("exp", None),
            P("exp", None),
            P("exp", None, "ctx"),
            P("exp", None, "ctx"),
            P("exp", None, "ctx"),
        ),
        out_specs=(P("ctx", "exp"), P("exp", "ctx")),
        check_vma=False,
    )
```
